32 devices in a mesh: fsdp: 16 (over z, x, core), tensor: 2 (over y).
Axes of the slice: x: 2, y: 2, z: 4, core: 2. Of those that a mesh axis runs over, the one named last changes fastest.
Arguments:
- tokens: bfloat16 [4096, 2048], P('fsdp'), may hold values from -6 to 6
- grad_out: bfloat16 [4096, 2048], P('fsdp'), may hold values from -6 to 6
- segments: int32 [32, 128], P('fsdp'), may hold values from 0 to 3, as said below
- attention_gain: float32 [2048], P('fsdp'), may hold values from 0.5 to 1.5
- query_weight: bfloat16 [2048, 2048], P('fsdp', 'tensor'), may hold values from -0.125 to 0.125
- key_weight: bfloat16 [2048, 1024], P('fsdp', 'tensor'), may hold values from -0.125 to 0.125
- value_weight: bfloat16 [2048, 1024], P('fsdp', 'tensor'), may hold values from -0.125 to 0.125
- output_weight: bfloat16 [2048, 2048], P('tensor', 'fsdp'), may hold values from -0.5 to 0.5
- query_gain: float32 [128], replicated, may hold values from 0.5 to 1.5
- key_gain: float32 [128], replicated, may hold values from 0.5 to 1.5
- feedforward_gain: float32 [2048], P('fsdp'), may hold values from 0.5 to 1.5
- gate_weight: bfloat16 [2048, 6144], P('fsdp', 'tensor'), may hold values from -0.125 to 0.125
- up_weight: bfloat16 [2048, 6144], P('fsdp', 'tensor'), may hold values from -0.125 to 0.125
- down_weight: bfloat16 [6144, 2048], P('tensor', 'fsdp'), may hold values from -0.078125 to 0.078125
Outputs:
- mixed: bfloat16 [4096, 2048], P('fsdp')
- grad_tokens: float32 [4096, 2048], P('fsdp')
- grad_attention_gain: float32 [2048], P('fsdp')
- grad_query_weight: float32 [2048, 2048], P('fsdp', 'tensor')
- grad_key_weight: float32 [2048, 1024], P('fsdp', 'tensor')
- grad_value_weight: float32 [2048, 1024], P('fsdp', 'tensor')
- grad_output_weight: float32 [2048, 2048], P('tensor', 'fsdp')
- grad_query_gain: float32 [128], replicated
- grad_key_gain: float32 [128], replicated
- grad_feedforward_gain: float32 [2048], P('fsdp')
- grad_gate_weight: float32 [2048, 6144], P('fsdp', 'tensor')
- grad_up_weight: float32 [2048, 6144], P('fsdp', 'tensor')
- grad_down_weight: float32 [6144, 2048], P('tensor', 'fsdp')
The draws below stay inside these ranges and needn't reach their ends.
Inputs may be any that keep to these rules, and one draw needn't show every extreme that they name: `segments`: segment numbers never fall along a row; every row holds one or more whole sequences, and some row is a single sequence of 128 tokens.
All inputs are finite; a program needn't handle non-finite values.
Results may differ from the reference program's by a relative error of at most 0.035.
Values may be sent and summed in bfloat16 or wider, within the bound.
A program may use at most 256 MiB of HBM per device.

```python
import jax
import jax.numpy as jnp
from jax import lax

D = 2048
H = 16
KV = 8
HD = 128
FF = 6144
MB_TOK = 128
CUTS = 3
TOKENS = 4096
BLOCKS = 32


def draw_segments(key, part):
    cut_key, whole_key, pick_key = jax.random.split(jax.random.fold_in(key, 11), 3)
    cut_points = jax.random.randint(cut_key, (BLOCKS, CUTS), 1, MB_TOK)
    whole_block = (jax.random.randint(whole_key, (BLOCKS,), 0, 4) == 0) | (jnp.arange(BLOCKS) == jax.random.randint(pick_key, (), 0, BLOCKS))
    cut_points = jnp.where(whole_block[:, None], MB_TOK, cut_points)
    slot_index = jnp.arange(MB_TOK)
    return jnp.sum(jnp.where(cut_points[:, None, :] <= slot_index[None, :, None], 1, 0), axis=-1).astype(jnp.int32)


def shard_levels(own_key, dims, cuts, low, largest):
    level, own = 1.0, jax.random.fold_in(own_key, 6)
    for dim, parts in cuts:
        draws = jnp.exp(jax.random.uniform(jax.random.fold_in(own, dim), (parts,), jnp.float32, low / len(cuts), largest / len(cuts)))
        level = level * jnp.repeat(draws, dims[dim] // parts).reshape([-1 if axis == dim else 1 for axis in range(len(dims))])
    return level


def noise(rng, extent, deviation, limit, cuts=(), dtype=jnp.bfloat16):
    result = deviation * jax.random.normal(rng, extent, jnp.float32)
    if cuts:
        result = result * shard_levels(rng, extent, cuts, -0.22, 0.18)
    return jnp.clip(result, -limit, limit).astype(dtype)


def setup_inputs(seed: int = 0) -> dict:
    key_list = jax.random.split(jax.random.key(seed), 15)
    tokens = noise(key_list[0], (TOKENS, D), 1.0, 6.0, ((0, 16),))
    grad_out = noise(key_list[1], (TOKENS, D), 1.0, 6.0, ((0, 16),))
    segments = draw_segments(jax.random.fold_in(key_list[14], 71), 0)
    attention_gain = jnp.clip(1.0 + 0.1 * jax.random.normal(key_list[3], (D,), jnp.float32), 0.5, 1.5)
    query_weight = noise(key_list[4], (D, H * HD), D ** -0.5, 0.125, ((0, 16), (1, 2)))
    key_weight = noise(key_list[5], (D, KV * HD), D ** -0.5, 0.125, ((0, 16), (1, 2)))
    value_weight = noise(key_list[6], (D, KV * HD), D ** -0.5, 0.125, ((0, 16), (1, 2)))
    output_weight = noise(key_list[7], (H * HD, D), (H * HD // 16) ** -0.5, 0.5, ((0, 2), (1, 16)))
    query_gain = jnp.clip(1.0 + 0.1 * jax.random.normal(key_list[8], (HD,), jnp.float32), 0.5, 1.5)
    key_gain = jnp.clip(1.0 + 0.1 * jax.random.normal(key_list[9], (HD,), jnp.float32), 0.5, 1.5)
    feedforward_gain = jnp.clip(1.0 + 0.1 * jax.random.normal(key_list[10], (D,), jnp.float32), 0.5, 1.5)
    gate_weight = noise(key_list[11], (D, FF), D ** -0.5, 0.125, ((0, 16), (1, 2)))
    up_weight = noise(key_list[12], (D, FF), D ** -0.5, 0.125, ((0, 16), (1, 2)))
    down_weight = noise(key_list[13], (FF, D), FF ** -0.5, 0.078125, ((0, 2), (1, 16)))
    return {"tokens": tokens, "grad_out": grad_out, "segments": segments, "attention_gain": attention_gain, "query_weight": query_weight, "key_weight": key_weight, "value_weight": value_weight, "output_weight": output_weight, "query_gain": query_gain, "key_gain": key_gain, "feedforward_gain": feedforward_gain, "gate_weight": gate_weight, "up_weight": up_weight, "down_weight": down_weight}


@jax.custom_vjp
def low(v):
    return lax.optimization_barrier(v.astype(jnp.bfloat16)).astype(jnp.float32)

@jax.custom_vjp
def low_back(v):
    return v

def low_keep(v):
    return (low(v), None)

def low_pass(kept, grad):
    return (grad,)

def back_keep(v):
    return (v, None)

def back_low(kept, grad):
    return (low(grad),)
low.defvjp(low_keep, low_pass)
low_back.defvjp(back_keep, back_low)
epsilon = 1e-06
rope_base = 1000000.0
highest = lax.Precision.HIGHEST

def matmul(left, right):
    return jnp.dot(left, right, precision=highest, preferred_element_type=jnp.float32)

def rms_norm(values):
    return values * lax.rsqrt(lax.optimization_barrier(jnp.mean(values * values, axis=-1, keepdims=True)) + epsilon)

def rotate(values, cosine, sine_table):
    half_size = values.shape[-1] // 2
    first = values[..., :half_size]
    second = values[..., half_size:]
    return jnp.concatenate([first * cosine - second * sine_table, second * cosine + first * sine_table], axis=-1)

def tables(segments):
    index_row = jnp.arange(MB_TOK)
    same_seg = segments[:, :, None] == segments[:, None, :]
    earlier = index_row[None, :, None] > index_row[None, None, :]
    position = lax.optimization_barrier(jnp.sum(jnp.where(same_seg & earlier, 1, 0), axis=-1)).astype(jnp.float32)
    allowed = same_seg & (index_row[None, :, None] >= index_row[None, None, :])
    frequency = rope_base ** (-2.0 * jnp.arange(HD // 2).astype(jnp.float32) / HD)
    angles = position.reshape(-1)[:, None] * frequency[None, :]
    return (jnp.cos(angles)[:, None, :], jnp.sin(angles)[:, None, :], allowed)

def attend(block_args):
    queries, key_heads, value_heads, allowed = block_args
    queries = queries.reshape(MB_TOK, KV, H // KV, HD)
    scores = low_back(jnp.einsum('qgrd,kgd->grqk', queries, key_heads, precision=highest) * HD ** (-0.5))
    scores = jnp.where(allowed[None, None], scores, -1e+30)
    attn_probs = low(jax.nn.softmax(scores, axis=-1))
    attended = jnp.einsum('grqk,kgd->qgrd', attn_probs, value_heads, precision=highest)
    return low(low_back(attended)).reshape(MB_TOK, H * HD)

def forward(tokens, attention_gain, query_weight, key_weight, value_weight, output_weight, query_gain, key_gain, feedforward_gain, gate_weight, up_weight, down_weight, cosine, sine_table, allowed):
    input_one = low(rms_norm(tokens) * attention_gain)
    query_raw = low_back(matmul(input_one, query_weight)).reshape(-1, H, HD)
    key_raw = low_back(matmul(input_one, key_weight)).reshape(-1, KV, HD)
    value_heads = low(low_back(matmul(input_one, value_weight))).reshape(BLOCKS, MB_TOK, KV, HD)
    queries = low(rotate(rms_norm(query_raw) * query_gain, cosine, sine_table)).reshape(BLOCKS, MB_TOK, H, HD)
    key_heads = low(rotate(rms_norm(key_raw) * key_gain, cosine, sine_table)).reshape(BLOCKS, MB_TOK, KV, HD)
    attended = lax.map(jax.checkpoint(attend), (queries, key_heads, value_heads, allowed)).reshape(-1, H * HD)
    residual = tokens + low_back(matmul(attended, output_weight))
    input_two = low(rms_norm(residual) * feedforward_gain)
    gate_pre = low_back(matmul(input_two, gate_weight))
    up_pre = low_back(matmul(input_two, up_weight))
    hidden = low(jax.nn.silu(gate_pre) * up_pre)
    return residual + low_back(matmul(hidden, down_weight))

def reference(tokens, grad_out, segments, attention_gain, query_weight, key_weight, value_weight, output_weight, query_gain, key_gain, feedforward_gain, gate_weight, up_weight, down_weight):
    cosine, sine_table, allowed = tables(segments)
    inputs = tuple((entry.astype(jnp.float32) for entry in (tokens, attention_gain, query_weight, key_weight, value_weight, output_weight, query_gain, key_gain, feedforward_gain, gate_weight, up_weight, down_weight)))

    def layer(*params):
        return forward(*params, cosine, sine_table, allowed)
    output, pullback = jax.vjp(layer, *inputs)
    grads = pullback(grad_out.astype(jnp.float32))
    return (output.astype(jnp.bfloat16), grads[0], grads[1], grads[2], grads[3], grads[4], grads[5], grads[6], grads[7], grads[8], grads[9], grads[10], grads[11])
```

```python
import jax
import jax.numpy as jnp
from jax import lax
from jax.sharding import Mesh
from jax.sharding import PartitionSpec as P


epsilon = 1e-06
rope_base = 1000000.0
bf16 = jnp.bfloat16
f32 = jnp.float32
pair = [(0, 1), (1, 0)]


def normalize(values):
    inverse = lax.rsqrt(jnp.mean(values * values, axis=-1, keepdims=True) + epsilon)
    return values * inverse, inverse


def norm_back(upstream, normed, inverse, gain):
    scaled = upstream * gain
    return inverse * (scaled - normed * jnp.mean(scaled * normed, axis=-1, keepdims=True))


def rotate(values, cosine, sine_table):
    half_size = values.shape[-1] // 2
    first = values[..., :half_size]
    second = values[..., half_size:]
    return jnp.concatenate(
        [first * cosine - second * sine_table, second * cosine + first * sine_table], axis=-1
    )


def dot(left, right):
    return jnp.dot(left, right, preferred_element_type=f32)


def dot_tn(left, right):
    return lax.dot_general(left, right, (((0,), (0,)), ((), ())), preferred_element_type=f32)


def dot_nt(left, right):
    return lax.dot_general(left, right, (((1,), (1,)), ((), ())), preferred_element_type=f32)


def tables(segments, head_size):
    index_row = jnp.arange(segments.shape[1])
    same_seg = segments[:, :, None] == segments[:, None, :]
    earlier = index_row[:, None] > index_row[None, :]
    position = jnp.sum(jnp.where(same_seg & earlier, 1, 0), axis=-1).astype(f32)
    allowed = same_seg & (index_row[:, None] >= index_row[None, :])
    frequency = rope_base ** (-2.0 * jnp.arange(head_size // 2).astype(f32) / head_size)
    angles = position[:, :, None] * frequency
    return jnp.cos(angles), jnp.sin(angles), allowed


def swap(values, axis):
    return lax.ppermute(values, axis, pair)


def across(values, axis):
    me = lax.axis_index(axis)
    kept = lax.dynamic_index_in_dim(values, me, 0, keepdims=False)
    sent = swap(lax.dynamic_index_in_dim(values, 1 - me, 0, keepdims=False), axis)
    first = me == 0
    return jnp.stack([jnp.where(first, kept, sent), jnp.where(first, sent, kept)])


def exchange(slabs):
    over_x = across(slabs, "x")
    return jnp.swapaxes(across(jnp.swapaxes(over_x, 0, 1), "core"), 0, 1)


def fetch(slabs):
    _, rows, columns = slabs.shape
    mine = exchange(slabs.reshape(2, 2, rows, columns)).reshape(4 * rows, columns)
    return lax.all_gather(mine, "z", axis=0, tiled=True)


def give_back(grads):
    summed = lax.psum_scatter(grads, "z", scatter_dimension=0, tiled=True)
    rows, columns = summed.shape[0] // 4, summed.shape[1]
    return exchange(summed.reshape(2, 2, rows, columns)).reshape(4, rows, columns)


def slabs_of(weight):
    rows, columns = weight.shape
    return jnp.swapaxes(weight.reshape(rows, 4, columns // 4), 0, 1)


def gather_rows(block):
    rows, width = block.shape
    half = rows // 2
    upper, lower = block[:half], block[half:]
    upper_x, lower_y = swap(upper, "x"), swap(lower, "y")
    upper_pair = jnp.stack([upper, upper_x])
    lower_pair = jnp.stack([lower, lower_y])
    upper_y = swap(upper_pair, "y")
    lower_x = swap(lower_pair, "x")
    quad_upper = jnp.stack([upper_pair, upper_y], axis=1)
    quad_lower = jnp.stack([lower_pair, lower_x], axis=0)
    quad = jnp.stack([quad_upper, quad_lower], axis=2).reshape(4 * rows, width)
    return jnp.concatenate([quad, swap(quad, "core")])


def scatter_rows(partial):
    width = partial.shape[1]
    rows = partial.shape[0] // 8
    half = rows // 2
    kept, sent = partial[: 4 * rows], partial[4 * rows :]
    quad = kept.astype(f32) + swap(sent, "core").astype(f32)
    quad = quad.astype(bf16).reshape(2, 2, 2, half, width)
    upper = quad[0, :, 0].astype(f32) + swap(quad[1, :, 0], "x").astype(f32)
    lower = quad[:, 0, 1].astype(f32) + swap(quad[:, 1, 1], "y").astype(f32)
    upper, lower = upper.astype(bf16), lower.astype(bf16)
    upper = upper[0].astype(f32) + swap(upper[1], "y").astype(f32)
    lower = lower[0].astype(f32) + swap(lower[1], "x").astype(f32)
    return jnp.concatenate([upper, lower])


def doubled(values, axes, combine):
    for axis, size in axes:
        step = 1
        while step < size:
            values = combine(
                values, lax.ppermute(values, axis, [(i, i ^ step) for i in range(size)]), axis, step
            )
            step *= 2
    return values


def total(values, depth):
    axes = (("core", 2), ("x", 2), ("y", 2), ("z", depth))
    return doubled(values, axes, lambda mine, other, axis, step: mine + other)


def gather_small(values, depth):
    def join(mine, other, axis, step):
        low = (lax.axis_index(axis) // step) % 2 == 0
        return jnp.concatenate([jnp.where(low, mine, other), jnp.where(low, other, mine)], axis=1)

    return doubled(values, (("core", 2), ("x", 2), ("z", depth)), join)


def own_first(values, mine):
    return jnp.where(mine == 0, values, values[::-1])


def attention_forward(qkv, shape, cosine, sine, allowed, query_gain, key_gain):
    blocks, rows, heads, groups, size = shape
    width_q, width_k = heads * size, groups * size
    ratio = heads // groups
    query_raw = qkv[:, :width_q].reshape(blocks, rows, heads, size)
    key_raw = qkv[:, width_q : width_q + width_k].reshape(blocks, rows, groups, size)
    value_heads = qkv[:, width_q + width_k :].astype(bf16).reshape(blocks, rows, groups, size)
    cosine, sine = cosine[:, :, None], sine[:, :, None]
    query_hat, query_inverse = normalize(query_raw)
    key_hat, key_inverse = normalize(key_raw)
    queries = rotate(query_hat * query_gain, cosine, sine).astype(bf16)
    queries = queries.reshape(blocks, rows, groups, ratio, size)
    key_heads = rotate(key_hat * key_gain, cosine, sine).astype(bf16)
    scores = jnp.einsum("bqgrd,bkgd->bgrqk", queries, key_heads, preferred_element_type=f32)
    scores = jnp.where(allowed[:, None, None], scores * size ** (-0.5), -1e30)
    peak = jnp.max(scores, axis=-1, keepdims=True)
    log_total = peak + jnp.log(jnp.sum(jnp.exp(scores - peak), axis=-1, keepdims=True))
    probs = jnp.exp(scores - log_total)
    attended = jnp.einsum(
        "bgrqk,bkgd->bqgrd", probs.astype(bf16), value_heads, preferred_element_type=f32
    )
    attended = attended.astype(bf16).reshape(blocks * rows, width_q)
    return attended, (
        query_hat, query_inverse, key_hat, key_inverse, queries, key_heads, value_heads, probs
    )


def attention_backward(d_attended, kept, cosine, sine, query_gain, key_gain):
    query_hat, query_inverse, key_hat, key_inverse, queries, key_heads, value_heads, probs = kept
    blocks, rows, groups, ratio, size = queries.shape
    scale = size ** (-0.5)
    cosine, sine = cosine[:, :, None], sine[:, :, None]
    d_attended = d_attended.reshape(blocks, rows, groups, ratio, size)
    d_value = jnp.einsum(
        "bgrqk,bqgrd->bkgd", probs.astype(bf16), d_attended, preferred_element_type=f32
    ).astype(bf16)
    d_probs = jnp.einsum("bqgrd,bkgd->bgrqk", d_attended, value_heads, preferred_element_type=f32)
    inner = jnp.sum(d_probs * probs, axis=-1, keepdims=True)
    d_scores = (probs * (d_probs - inner)).astype(bf16)
    d_queries = scale * jnp.einsum(
        "bgrqk,bkgd->bqgrd", d_scores, key_heads, preferred_element_type=f32
    ).reshape(blocks, rows, groups * ratio, size)
    d_keys = scale * jnp.einsum(
        "bgrqk,bqgrd->bkgd", d_scores, queries, preferred_element_type=f32
    )
    d_query_rot = rotate(d_queries, cosine, -sine)
    d_key_rot = rotate(d_keys, cosine, -sine)
    grad_query_gain = jnp.sum(d_query_rot * query_hat, axis=(0, 1, 2))
    grad_key_gain = jnp.sum(d_key_rot * key_hat, axis=(0, 1, 2))
    d_query_raw = norm_back(d_query_rot, query_hat, query_inverse, query_gain).astype(bf16)
    d_key_raw = norm_back(d_key_rot, key_hat, key_inverse, key_gain).astype(bf16)
    flat = [
        part.reshape(blocks * rows, -1) for part in (d_query_raw, d_key_raw, d_value)
    ]
    return jnp.concatenate(flat, axis=1), grad_query_gain, grad_key_gain


def on_device(depth, tokens, grad_out, segments, attention_gain, query_weight, key_weight,
              value_weight, output_weight, query_gain, key_gain, feedforward_gain, gate_weight,
              up_weight, down_weight):
    size = query_gain.shape[0]
    blocks, rows = segments.shape
    width = tokens.shape[1]
    heads = query_weight.shape[1] // size // 4
    groups = key_weight.shape[1] // size // 4
    shape = (8 * blocks // 2, rows, heads, groups, size)
    mine = lax.axis_index("y")
    place = lax.axis_index("z") * 4 + lax.axis_index("x") * 2 + lax.axis_index("core")

    attention_slabs = jnp.concatenate(
        [slabs_of(w) for w in (query_weight, key_weight, value_weight, output_weight.T)], axis=2
    )
    widths = [w.shape[1] // 4 for w in (query_weight, key_weight, value_weight)]
    width_qkv = sum(widths)
    attention_all = fetch(attention_slabs)
    qkv_weight, output_all = attention_all[:, :width_qkv], attention_all[:, width_qkv:]
    gate_up_all = fetch(jnp.concatenate([slabs_of(gate_weight), slabs_of(up_weight)], axis=2))
    down_all = fetch(slabs_of(down_weight.T))
    hidden_size = down_all.shape[1]

    gains = gather_small(jnp.stack([attention_gain, feedforward_gain]), depth)
    attention_gain_all, feedforward_gain_all = gains[0], gains[1]

    token_pair = own_first(tokens.reshape(2, -1, width), mine)
    grad_pair = own_first(grad_out.reshape(2, -1, width), mine)
    segment_pair = own_first(segments.reshape(2, -1, rows), mine)

    def gather_pairs(pairs):
        both = jnp.stack([pairs, swap(pairs, "x")])
        return jnp.stack([both, swap(both, "core")]).reshape(-1, pairs.shape[-1])

    inputs = token_pair.astype(f32)
    normed_pair, inverse_pair = normalize(inputs)
    input_one = gather_pairs((normed_pair * attention_gain_all).astype(bf16))
    segments_all = gather_pairs(segment_pair)
    grads_all = gather_pairs(grad_pair)
    residual_in, normed_one, inverse_one = inputs[0], normed_pair[0], inverse_pair[0]
    cosine, sine, allowed = tables(segments_all, size)

    qkv = dot(input_one, qkv_weight)
    attended, kept = attention_forward(qkv, shape, cosine, sine, allowed, query_gain, key_gain)
    residual = residual_in + scatter_rows(dot_nt(attended, output_all).astype(bf16))
    normed_two, inverse_two = normalize(residual)
    input_two = gather_rows((normed_two * feedforward_gain_all).astype(bf16))
    gate_up = dot(input_two, gate_up_all)
    gate_pre, up_pre = gate_up[:, :hidden_size], gate_up[:, hidden_size:]
    sigma = jax.nn.sigmoid(gate_pre)
    hidden = (gate_pre * sigma * up_pre).astype(bf16)

    grad_down = give_back(dot_tn(grads_all, hidden).astype(bf16))
    d_hidden = dot(grads_all, down_all)
    d_gate = (d_hidden * up_pre * sigma * (1.0 + gate_pre * (1.0 - sigma))).astype(bf16)
    d_up = (d_hidden * gate_pre * sigma).astype(bf16)
    d_gate_up = jnp.concatenate([d_gate, d_up], axis=1)
    d_input_two = scatter_rows(dot_nt(d_gate_up, gate_up_all).astype(bf16))
    grad_gate_up = give_back(dot_tn(input_two, d_gate_up).astype(bf16))

    mixed_own = (residual + scatter_rows(dot_nt(hidden, down_all).astype(bf16))).astype(bf16)
    mixed = own_first(jnp.stack([mixed_own, swap(mixed_own, "y")]), mine).reshape(-1, width)

    grad_two = jnp.sum(d_input_two * normed_two, axis=0)
    d_residual = grad_pair[0].astype(f32) + norm_back(
        d_input_two, normed_two, inverse_two, feedforward_gain_all
    )
    d_residual_low = gather_rows(d_residual.astype(bf16))
    d_attended = dot(d_residual_low, output_all).astype(bf16)
    d_qkv, grad_query_gain, grad_key_gain = attention_backward(
        d_attended, kept, cosine, sine, query_gain, key_gain
    )
    grad_attention = jnp.concatenate(
        [dot_tn(input_one, d_qkv).astype(bf16), dot_tn(d_residual_low, attended).astype(bf16)],
        axis=1,
    )
    grad_attention = give_back(grad_attention)
    d_input_one = scatter_rows(dot_nt(d_qkv, qkv_weight).astype(bf16))
    grad_one = jnp.sum(d_input_one * normed_one, axis=0)
    d_tokens = d_residual + norm_back(d_input_one, normed_one, inverse_one, attention_gain_all)
    grad_tokens = own_first(jnp.stack([d_tokens, swap(d_tokens, "y")]), mine).reshape(-1, width)

    early = total(
        jnp.concatenate([grad_two, grad_query_gain, grad_key_gain]).reshape(1, -1), depth
    )[0]
    late = total(grad_one.reshape(1, -1), depth)[0]
    rows_here = attention_gain.shape[0]
    start = place * rows_here
    grad_attention_gain = lax.dynamic_slice(late, (start,), (rows_here,))
    grad_feedforward_gain = lax.dynamic_slice(early, (start,), (rows_here,))

    def columns(slabs):
        return jnp.swapaxes(slabs, 0, 1).reshape(slabs.shape[1], -1).astype(f32)

    bounds = [0]
    for w in widths:
        bounds.append(bounds[-1] + w)
    grad_query, grad_key, grad_value = (
        columns(grad_attention[:, :, bounds[i] : bounds[i + 1]]) for i in range(3)
    )
    grad_output = columns(grad_attention[:, :, width_qkv:]).T
    return (
        mixed,
        grad_tokens,
        grad_attention_gain,
        grad_query,
        grad_key,
        grad_value,
        grad_output,
        early[width : width + size],
        early[width + size :],
        grad_feedforward_gain,
        columns(grad_gate_up[:, :, :hidden_size]),
        columns(grad_gate_up[:, :, hidden_size:]),
        columns(grad_down).T,
    )


def solution(mesh):
    shards = mesh.shape["fsdp"]
    depth = shards // 4
    fine = Mesh(
        mesh.devices.reshape(depth, 2, 2, mesh.shape["tensor"]), ("z", "x", "core", "y")
    )
    fsdp = ("z", "x", "core")
    whole, both, turned, flat = P(fsdp, None), P(fsdp, "y"), P("y", fsdp), P(fsdp)

    def step(*arrays):
        return on_device(depth, *arrays)

    return jax.shard_map(
        step,
        mesh=fine,
        in_specs=(
            whole, whole, whole, flat, both, both, both, turned, P(), P(), flat, both, both, turned
        ),
        out_specs=(
            whole, whole, flat, both, both, both, turned, P(), P(), flat, both, both, turned
        ),
        check_vma=False,
    )
```

```python
import functools

import jax
import jax.numpy as jnp
from jax import lax
from jax.experimental import pallas as pl
from jax.experimental.pallas import tpu as pltpu
from jax.sharding import Mesh
from jax.sharding import PartitionSpec as P


epsilon = 1e-06
rope_base = 1000000.0
bf16 = jnp.bfloat16
f32 = jnp.float32
pair = [(0, 1), (1, 0)]
MESH = pl.DeviceIdType.MESH
bits = {"zl": 4, "x": 2, "y": 1}
orders = (("x", "y", "zl"), ("y", "zl", "x"), ("zl", "x", "y"))
chunk = 16


def normalize(values):
    inverse = lax.rsqrt(jnp.mean(values * values, axis=-1, keepdims=True) + epsilon)
    return values * inverse, inverse


def norm_back(upstream, normed, inverse):
    return inverse * (upstream - normed * jnp.mean(upstream * normed, axis=-1, keepdims=True))


def rotate(values, cosine, sine_table):
    half_size = values.shape[-1] // 2
    first = values[..., :half_size]
    second = values[..., half_size:]
    return jnp.concatenate(
        [first * cosine - second * sine_table, second * cosine + first * sine_table], axis=-1
    )


def dot(left, right):
    return jnp.dot(left, right, preferred_element_type=f32)


def dot_tn(left, right):
    return lax.dot_general(left, right, (((0,), (0,)), ((), ())), preferred_element_type=f32)


def dot_nt(left, right):
    return lax.dot_general(left, right, (((1,), (1,)), ((), ())), preferred_element_type=f32)


def parts_of(width):
    tiles = width // 128
    first, second = tiles // 3, 2 * (tiles // 3)
    edges = (0, first * 128, second * 128, width)
    return [pl.ds(edges[i], edges[i + 1] - edges[i]) for i in range(3)]


def greet():
    barrier = pltpu.get_barrier_semaphore()
    for axis in bits:
        pl.semaphore_signal(
            barrier, inc=1, device_id={axis: 1 - lax.axis_index(axis)}, device_id_type=MESH
        )
    pl.semaphore_wait(barrier, 3)


def copy_to(axis, source, target, sems, number):
    return pltpu.make_async_remote_copy(
        src_ref=source,
        dst_ref=target,
        send_sem=sems[0].at[number],
        recv_sem=sems[1].at[number],
        device_id={axis: 1 - lax.axis_index(axis)},
        device_id_type=MESH,
    )


def gather_start(blocks, sems):
    parts = parts_of(blocks.shape[2])
    copies = {}

    def send(p, axis, i):
        number = len(copies)
        copies[p, axis, i] = copy_to(
            axis,
            blocks.at[i, :, parts[p]],
            blocks.at[i ^ bits[axis], :, parts[p]],
            sems,
            number,
        )
        copies[p, axis, i].start()

    for place in range(3):
        for p in range(3):
            send(p, orders[p][place], 0)
    return copies, send


def gather_finish(copies, send):
    for p in range(3):
        a, b, c = orders[p]
        copies[p, a, 0].wait_recv()
        send(p, b, bits[a])
        send(p, c, bits[a])
    for p in range(3):
        a, b, c = orders[p]
        copies[p, b, 0].wait_recv()
        send(p, c, bits[b])
        copies[p, b, bits[a]].wait_recv()
        send(p, c, bits[a] ^ bits[b])
    for p in range(3):
        a, b, c = orders[p]
        for i in (0, bits[a], bits[b], bits[a] ^ bits[b]):
            copies[p, c, i].wait_recv()
    for copy in copies.values():
        copy.wait_send()


def over_rows(rows, body):
    def step(i, carry):
        body(pl.ds(pl.multiple_of(i * chunk, chunk), chunk))
        return carry

    lax.fori_loop(0, rows // chunk, step, 0)


def scatter(blocks, first, second, third, sent, sems):
    rows, width = blocks.shape[1:]
    parts = parts_of(width)
    copies = []

    def send(axis, source, target):
        copies.append(copy_to(axis, source, target, sems, len(copies)))
        copies[-1].start()
        return copies[-1]

    arrive = {}
    for k in (3, 2, 1, 0):
        for p in range(3):
            a, b, c = orders[p]
            j = (bits[a] if k & 1 else 0) ^ (bits[b] if k & 2 else 0)
            arrive[p, k] = send(
                c, blocks.at[j ^ bits[c], :, parts[p]], first.at[k, :, parts[p]]
            )
    for k in (3, 2):
        for p in range(3):
            a, b, c = orders[p]
            j = (bits[a] if k & 1 else 0) ^ bits[b]
            arrive[p, k].wait_recv()

            def add(row, j=j, k=k, p=p):
                value = blocks[j, row, parts[p]].astype(f32) + first[k, row, parts[p]].astype(f32)
                sent[k - 1, row, parts[p]] = value.astype(bf16)

            over_rows(rows, add)
            arrive[p, k + 2] = send(
                b, sent.at[k - 1, :, parts[p]], second.at[k - 2, :, parts[p]]
            )
    for p in range(3):
        a, b, c = orders[p]
        arrive[p, 1].wait_recv()
        arrive[p, 5].wait_recv()

        def add(row, j=bits[a], p=p):
            value = blocks[j, row, parts[p]].astype(f32) + first[1, row, parts[p]].astype(f32)
            value = value + second[1, row, parts[p]].astype(f32)
            sent[0, row, parts[p]] = value.astype(bf16)

        over_rows(rows, add)
        arrive[p, 6] = send(a, sent.at[0, :, parts[p]], third.at[0, :, parts[p]])
    for p in range(3):
        for k in (0, 4, 6):
            arrive[p, k].wait_recv()
    for copy in copies:
        copy.wait_send()


def summed(row, blocks, first, second, third):
    value = blocks[0, row].astype(f32) + first[0, row].astype(f32)
    return value + second[0, row].astype(f32) + third[0, row].astype(f32)


def scatter_scratch(rows, width):
    return [
        pltpu.VMEM((4, rows, width), bf16),
        pltpu.VMEM((2, rows, width), bf16),
        pltpu.VMEM((1, rows, width), bf16),
        pltpu.VMEM((3, rows, width), bf16),
        pltpu.SemaphoreType.DMA((21,)),
        pltpu.SemaphoreType.DMA((21,)),
    ]


def gather_scratch():
    return [pltpu.SemaphoreType.DMA((21,)), pltpu.SemaphoreType.DMA((21,))]


def call(kernel, number, outputs, scratch, *operands, name=None):
    return pl.pallas_call(
        kernel,
        out_shape=outputs,
        in_specs=[pl.BlockSpec(memory_space=pltpu.VMEM)] * len(operands),
        out_specs=jax.tree.map(lambda _: pl.BlockSpec(memory_space=pltpu.VMEM), outputs),
        scratch_shapes=scratch,
        compiler_params=pltpu.CompilerParams(collective_id=number, has_side_effects=True),
        name=name,
    )(*operands)


def permuted(depth, count, tile):
    places = []
    for block in range(count):
        high, rest = divmod(block, 8)
        places.append(high * 8 + rest % 2 * 4 + rest // 2)
    return places if tile % 128 == 0 else list(range(count))


def put(ref, index, row, value, places):
    tile = value.shape[1] // len(places)
    if places == sorted(places):
        ref[index, row] = value
        return
    for block, place in enumerate(places):
        ref[index, row, pl.ds(place * tile, tile)] = value[:, block * tile : (block + 1) * tile]


def straight(value, places):
    if places == sorted(places):
        return value
    tile = value.shape[1] // len(places)
    return jnp.concatenate(
        [value[:, place * tile : (place + 1) * tile] for place in places], axis=1
    )


def cube_id(step):
    high, low = lax.axis_index("zl"), lax.axis_index("x")
    return {"zl": 1 - high if step & 2 else high, "x": 1 - low if step & 1 else low}


def square_place(step):
    device = cube_id(step)
    return device["zl"] * 2 + device["x"]


def greet_square(others=()):
    barrier = pltpu.get_barrier_semaphore()
    for step in (1, 2, 3):
        pl.semaphore_signal(barrier, inc=1, device_id=cube_id(step), device_id_type=MESH)
    for axis in others:
        pl.semaphore_signal(
            barrier, inc=1, device_id={axis: 1 - lax.axis_index(axis)}, device_id_type=MESH
        )
    pl.semaphore_wait(barrier, 3 + len(others))


def spread_start(sources, targets, sems):
    copies = []
    me = square_place(0)
    for n, (source, target) in enumerate(zip(sources, targets)):
        for step in (3, 1, 2):
            copies.append(
                pltpu.make_async_remote_copy(
                    src_ref=source.at[square_place(step)],
                    dst_ref=target.at[me],
                    send_sem=sems[0].at[n, step],
                    recv_sem=sems[1].at[n, step],
                    device_id=cube_id(step),
                    device_id_type=MESH,
                )
            )
        copies.append(pltpu.make_async_copy(source.at[me], target.at[me], sems[0].at[n, 0]))
    for copy in copies:
        copy.start()
    return copies


def spread_scratch(count):
    return [pltpu.SemaphoreType.DMA((count, 4)), pltpu.SemaphoreType.DMA((count, 4))]


def enter_kernel(places, slabs_one, slabs_two, tokens, spread_one, spread_two, inputs_all, *sems):
    greet_square(("y",))
    copies = spread_start((slabs_one, slabs_two), (spread_one, spread_two), sems[:2])

    def norm(row):
        normed, _ = normalize(tokens[row].astype(f32))
        put(inputs_all, 0, row, normed.astype(bf16), places)

    over_rows(tokens.shape[0], norm)
    gather_finish(*gather_start(inputs_all, sems[2:]))
    for copy in copies:
        copy.wait()


def spread_kernel(slabs_one, slabs_two, spread_one, spread_two, *sems):
    greet_square()
    for copy in spread_start((slabs_one, slabs_two), (spread_one, spread_two), sems):
        copy.wait()


def grads_kernel(places, grads, grads_all, *sems):
    greet()

    def load(row):
        put(grads_all, 0, row, grads[row], places)

    over_rows(grads.shape[0], load)
    gather_finish(*gather_start(grads_all, sems))


def middle_kernel(places, partial, tokens, residual, inputs_all, *scratch):
    greet()
    buffers, sems, gather_sems = scratch[:3], scratch[4:6], scratch[6:8]
    scatter(partial, *buffers, scratch[3], sems)

    def norm(row):
        value = straight(summed(row, partial, *buffers), places) + tokens[row].astype(f32)
        residual[row] = value
        put(inputs_all, 0, row, normalize(value)[0].astype(bf16), places)

    over_rows(tokens.shape[0], norm)
    gather_finish(*gather_start(inputs_all, gather_sems))


def back_kernel(places, partial, residual, grads, d_residual, low_all, *scratch):
    greet()
    buffers, sems, gather_sems = scratch[:3], scratch[4:6], scratch[6:8]
    scatter(partial, *buffers, scratch[3], sems)

    def norm(row):
        normed, inverse = normalize(residual[row])
        value = grads[row].astype(f32) + norm_back(
            straight(summed(row, partial, *buffers), places), normed, inverse
        )
        d_residual[row] = value
        put(low_all, 0, row, value.astype(bf16), places)

    over_rows(residual.shape[0], norm)
    gather_finish(*gather_start(low_all, gather_sems))


def swap_rows(both, mine, sems):
    copy = copy_to("y", both.at[mine], both.at[mine], sems, 0)
    copy.start()
    copy.wait()


def leave_kernel(places, partial, tokens, d_residual, both, *scratch):
    greet()
    buffers, sems = scratch[:3], scratch[4:6]
    mine = lax.axis_index("y")
    scatter(partial, *buffers, scratch[3], sems)

    def norm(row):
        normed, inverse = normalize(tokens[row].astype(f32))
        value = d_residual[row] + norm_back(
            straight(summed(row, partial, *buffers), places), normed, inverse
        )
        both[mine, row] = value.astype(bf16)

    over_rows(tokens.shape[0], norm)
    swap_rows(both, mine, scratch[6:8])


def mixed_kernel(places, partial, residual, both, *scratch):
    greet()
    buffers, sems = scratch[:3], scratch[4:6]
    mine = lax.axis_index("y")
    scatter(partial, *buffers, scratch[3], sems)

    def add(row):
        value = residual[row] + straight(summed(row, partial, *buffers), places)
        both[mine, row] = value.astype(bf16)

    over_rows(residual.shape[0], add)
    swap_rows(both, mine, scratch[6:8])


def tables(segments, head_size):
    index_row = jnp.arange(segments.shape[1])
    same_seg = segments[:, :, None] == segments[:, None, :]
    earlier = index_row[:, None] > index_row[None, :]
    position = jnp.sum(jnp.where(same_seg & earlier, 1, 0), axis=-1).astype(f32)
    allowed = same_seg & (index_row[:, None] >= index_row[None, :])
    frequency = rope_base ** (-2.0 * jnp.arange(head_size // 2).astype(f32) / head_size)
    angles = position[:, :, None] * frequency
    return jnp.cos(angles), jnp.sin(angles), allowed


def swap(values, axis):
    return lax.ppermute(values, axis, pair)


def tidy(rows, depth, places, back):
    if places != sorted(places):
        return rows
    columns = rows.shape[1]
    inner = (4, 2) if back else (2, 4)
    rows = rows.reshape(depth, *inner, -1, columns)
    return jnp.swapaxes(rows, 1, 2).reshape(-1, columns)


def fetch(spread, depth, places):
    columns = spread.shape[2]
    rows = lax.all_gather(spread.reshape(-1, columns), ("zh", "core"), axis=0, tiled=True)
    return tidy(rows, depth, places, False)


def give_back(grads, depth, places):
    grads = tidy(grads, depth, places, True)
    summed_rows = lax.psum_scatter(grads, ("zh", "core"), scatter_dimension=0, tiled=True)
    return summed_rows.reshape(4, -1, grads.shape[1])


def slabs_of(weight):
    rows, columns = weight.shape
    return jnp.swapaxes(weight.reshape(rows, 4, columns // 4), 0, 1)


def total_of(values, depth):
    for axis, size in (("core", 2), ("x", 2), ("y", 2), ("zl", 2), ("zh", depth)):
        step = 1
        while step < size:
            values = values + lax.ppermute(values, axis, [(i, i ^ step) for i in range(size)])
            step *= 2
    return values


def attention_forward(qkv, shape, cosine, sine, allowed, query_gain, key_gain):
    blocks, rows, heads, groups, size = shape
    width_q, width_k = heads * size, groups * size
    ratio = heads // groups
    query_raw = qkv[:, :width_q].reshape(blocks, rows, heads, size)
    key_raw = qkv[:, width_q : width_q + width_k].reshape(blocks, rows, groups, size)
    value_heads = qkv[:, width_q + width_k :].astype(bf16).reshape(blocks, rows, groups, size)
    cosine, sine = cosine[:, :, None], sine[:, :, None]
    query_hat, query_inverse = normalize(query_raw)
    key_hat, key_inverse = normalize(key_raw)
    queries = rotate(query_hat * query_gain, cosine, sine).astype(bf16)
    queries = queries.reshape(blocks, rows, groups, ratio, size)
    key_heads = rotate(key_hat * key_gain, cosine, sine).astype(bf16)
    scores = jnp.einsum("bqgrd,bkgd->bgrqk", queries, key_heads, preferred_element_type=f32)
    scores = jnp.where(allowed[:, None, None], scores * size ** (-0.5), -1e30)
    peak = jnp.max(scores, axis=-1, keepdims=True)
    log_total = peak + jnp.log(jnp.sum(jnp.exp(scores - peak), axis=-1, keepdims=True))
    probs = jnp.exp(scores - log_total)
    attended = jnp.einsum(
        "bgrqk,bkgd->bqgrd", probs.astype(bf16), value_heads, preferred_element_type=f32
    )
    attended = attended.astype(bf16).reshape(blocks * rows, width_q)
    return attended, (
        query_hat, query_inverse, key_hat, key_inverse, queries, key_heads, value_heads, probs
    )


def attention_backward(d_attended, kept, cosine, sine, query_gain, key_gain):
    query_hat, query_inverse, key_hat, key_inverse, queries, key_heads, value_heads, probs = kept
    blocks, rows, groups, ratio, size = queries.shape
    scale = size ** (-0.5)
    cosine, sine = cosine[:, :, None], sine[:, :, None]
    d_attended = d_attended.reshape(blocks, rows, groups, ratio, size)
    d_value = jnp.einsum(
        "bgrqk,bqgrd->bkgd", probs.astype(bf16), d_attended, preferred_element_type=f32
    ).astype(bf16)
    d_probs = jnp.einsum("bqgrd,bkgd->bgrqk", d_attended, value_heads, preferred_element_type=f32)
    inner = jnp.sum(d_probs * probs, axis=-1, keepdims=True)
    d_scores = (probs * (d_probs - inner)).astype(bf16)
    d_queries = scale * jnp.einsum(
        "bgrqk,bkgd->bqgrd", d_scores, key_heads, preferred_element_type=f32
    ).reshape(blocks, rows, groups * ratio, size)
    d_keys = scale * jnp.einsum(
        "bgrqk,bqgrd->bkgd", d_scores, queries, preferred_element_type=f32
    )
    d_query_rot = rotate(d_queries, cosine, -sine)
    d_key_rot = rotate(d_keys, cosine, -sine)
    grad_query_gain = jnp.sum(d_query_rot * query_hat, axis=(0, 1, 2))
    grad_key_gain = jnp.sum(d_key_rot * key_hat, axis=(0, 1, 2))
    d_query_raw = norm_back(d_query_rot * query_gain, query_hat, query_inverse).astype(bf16)
    d_key_raw = norm_back(d_key_rot * key_gain, key_hat, key_inverse).astype(bf16)
    flat = [
        part.reshape(blocks * rows, -1) for part in (d_query_raw, d_key_raw, d_value)
    ]
    return jnp.concatenate(flat, axis=1), grad_query_gain, grad_key_gain


def on_device(depth, tokens, grad_out, segments, attention_gain, query_weight, key_weight,
              value_weight, output_weight, query_gain, key_gain, feedforward_gain, gate_weight,
              up_weight, down_weight):
    size = query_gain.shape[0]
    blocks, rows = segments.shape
    width = tokens.shape[1]
    rows_here = attention_gain.shape[0]
    heads = query_weight.shape[1] // size // 4
    groups = key_weight.shape[1] // size // 4
    shape = (8 * blocks // 2, rows, heads, groups, size)
    mine = lax.axis_index("y")
    gain_one, gain_two = attention_gain[:, None], feedforward_gain[:, None]

    def scaled(weight, gain):
        return (weight.astype(f32) * gain).astype(bf16)

    def own(values):
        return lax.dynamic_index_in_dim(
            values.reshape(2, -1, values.shape[-1]), mine, 0, keepdims=False
        )

    count = width // rows_here
    places = permuted(depth, count, rows_here)

    def shaped(array):
        return jax.ShapeDtypeStruct(array.shape, array.dtype)

    def with_places(kernel):
        return functools.partial(kernel, places)

    qkv_slabs = jnp.concatenate(
        [slabs_of(scaled(w, gain_one)) for w in (query_weight, key_weight, value_weight)], axis=2
    )
    output_slabs = slabs_of(output_weight.T)
    gate_up_slabs = jnp.concatenate(
        [slabs_of(scaled(w, gain_two)) for w in (gate_weight, up_weight)], axis=2
    )
    down_slabs = slabs_of(down_weight.T)
    hidden_size = down_slabs.shape[2]

    token_own, grad_own = own(tokens), own(grad_out)
    block_rows = token_own.shape[0]
    block = jax.ShapeDtypeStruct((block_rows, width), f32)
    everyone = jax.ShapeDtypeStruct((8, block_rows, width), bf16)

    def scatter_shapes():
        return scatter_scratch(block_rows, width)

    qkv_slabs, output_slabs, input_one = call(
        with_places(enter_kernel),
        1,
        (shaped(qkv_slabs), shaped(output_slabs), everyone),
        spread_scratch(2) + gather_scratch(),
        qkv_slabs,
        output_slabs,
        token_own,
        name="enter",
    )
    input_one = input_one.reshape(-1, width)
    qkv_weight = fetch(qkv_slabs, depth, places)
    output_all = fetch(output_slabs, depth, places)
    gate_up_slabs, down_slabs, _ = lax.optimization_barrier(
        (gate_up_slabs, down_slabs, input_one)
    )
    gate_up_slabs, down_slabs = call(
        spread_kernel,
        6,
        (shaped(gate_up_slabs), shaped(down_slabs)),
        spread_scratch(2),
        gate_up_slabs,
        down_slabs,
        name="spread",
    )
    gate_up_all = fetch(gate_up_slabs, depth, places)
    down_all = fetch(down_slabs, depth, places)

    pairs = jnp.where(mine == 0, segments.reshape(2, -1, rows), segments.reshape(2, -1, rows)[::-1])
    quads = jnp.stack([pairs, swap(pairs, "x")])
    segments_all = jnp.stack([quads, swap(quads, "zl")]).reshape(-1, rows)
    cosine, sine, allowed = tables(segments_all, size)

    qkv = dot(input_one, qkv_weight)
    attended, kept = attention_forward(qkv, shape, cosine, sine, allowed, query_gain, key_gain)
    partial = dot_nt(attended, output_all).astype(bf16).reshape(8, -1, width)
    residual, input_two = call(
        with_places(middle_kernel),
        2,
        (block, everyone),
        scatter_shapes() + gather_scratch(),
        partial,
        token_own,
        name="middle",
    )
    input_two = input_two.reshape(-1, width)
    grad_own, _ = lax.optimization_barrier((grad_own, residual))
    grads_all = call(
        with_places(grads_kernel), 7, everyone, gather_scratch(), grad_own, name="grads"
    ).reshape(-1, width)

    gate_up = dot(input_two, gate_up_all)
    gate_pre, up_pre = gate_up[:, :hidden_size], gate_up[:, hidden_size:]
    sigma = jax.nn.sigmoid(gate_pre)
    hidden = (gate_pre * sigma * up_pre).astype(bf16)
    grad_down = dot_tn(grads_all, hidden).astype(bf16)
    grad_down = give_back(grad_down, depth, places)
    d_hidden = dot(grads_all, down_all)
    d_gate = (d_hidden * up_pre * sigma * (1.0 + gate_pre * (1.0 - sigma))).astype(bf16)
    d_up = (d_hidden * gate_pre * sigma).astype(bf16)
    d_gate_up = jnp.concatenate([d_gate, d_up], axis=1)
    grad_gate_up = dot_tn(input_two, d_gate_up).astype(bf16)
    partial = dot_nt(d_gate_up, gate_up_all).astype(bf16).reshape(8, -1, width)
    grad_gate_up, partial = lax.optimization_barrier((grad_gate_up, partial))
    d_residual, d_residual_low = call(
        with_places(back_kernel),
        3,
        (block, everyone),
        scatter_shapes() + gather_scratch(),
        partial,
        residual,
        grad_own,
        name="back",
    )
    d_residual_low = d_residual_low.reshape(-1, width)
    grad_gate_up = give_back(grad_gate_up, depth, places)

    d_attended = dot(d_residual_low, output_all).astype(bf16)
    grad_output = give_back(dot_tn(d_residual_low, attended).astype(bf16), depth, places)
    d_qkv, grad_query_gain, grad_key_gain = attention_backward(
        d_attended, kept, cosine, sine, query_gain, key_gain
    )
    grad_qkv = dot_tn(input_one, d_qkv).astype(bf16)
    partial = dot_nt(d_qkv, qkv_weight).astype(bf16).reshape(8, -1, width)
    grad_qkv, partial = lax.optimization_barrier((grad_qkv, partial))
    grad_qkv = give_back(grad_qkv, depth, places)
    y_sems = [pltpu.SemaphoreType.DMA((1,)), pltpu.SemaphoreType.DMA((1,))]
    both = jax.ShapeDtypeStruct((2, block_rows, width), bf16)
    grad_tokens = call(
        with_places(leave_kernel),
        4,
        both,
        scatter_shapes() + y_sems,
        partial,
        token_own,
        d_residual,
        name="leave",
    ).reshape(-1, width)

    late, _ = lax.optimization_barrier((hidden, grad_tokens))
    partial = dot_nt(late, down_all).astype(bf16).reshape(8, -1, width)
    mixed = call(
        with_places(mixed_kernel),
        5,
        both,
        scatter_shapes() + y_sems,
        partial,
        residual,
        name="mixed",
    ).reshape(-1, width)

    def collect(one, two, number, after):
        one, two, _ = lax.optimization_barrier((one, two, after))
        return call(
            spread_kernel,
            number,
            (shaped(one), shaped(two)),
            spread_scratch(2),
            one,
            two,
            name="collect",
        )

    grad_gate_up, grad_down = collect(grad_gate_up, grad_down, 8, mixed)
    grad_qkv, grad_output = collect(grad_qkv, grad_output, 9, grad_gate_up)
    grad_tokens = grad_tokens.astype(f32)

    head_gains = total_of(jnp.concatenate([grad_query_gain, grad_key_gain]).reshape(2, -1), depth)

    def columns(slabs, start, stop):
        part = slabs[:, :, start:stop]
        return jnp.swapaxes(part, 0, 1).reshape(part.shape[1], -1).astype(f32)

    def finish(raw, weights, gain):
        gain_sums = sum(jnp.sum(w.astype(f32) * g, axis=1) for w, g in zip(weights, raw))
        return [g * gain for g in raw], gain_sums

    bounds = [0]
    for w in (query_weight, key_weight, value_weight):
        bounds.append(bounds[-1] + w.shape[1] // 4)
    raw = [columns(grad_qkv, bounds[i], bounds[i + 1]) for i in range(3)]
    (grad_query, grad_key, grad_value), sum_one = finish(
        raw, (query_weight, key_weight, value_weight), gain_one
    )
    raw = [columns(grad_gate_up, i * hidden_size, (i + 1) * hidden_size) for i in range(2)]
    (grad_gate, grad_up), sum_two = finish(raw, (gate_weight, up_weight), gain_two)
    sum_one = sum_one.reshape(1, rows_here)
    sum_two = sum_two.reshape(1, rows_here)
    return (
        mixed,
        grad_tokens,
        (sum_one + swap(sum_one, "y"))[0],
        grad_query,
        grad_key,
        grad_value,
        columns(grad_output, 0, None).T,
        head_gains[0],
        head_gains[1],
        (sum_two + swap(sum_two, "y"))[0],
        grad_gate,
        grad_up,
        columns(grad_down, 0, None).T,
    )


def solution(mesh):
    depth = mesh.shape["fsdp"] // 8
    fine = Mesh(
        mesh.devices.reshape(depth, 2, 2, 2, mesh.shape["tensor"]),
        ("zh", "zl", "x", "core", "y"),
    )
    fsdp = ("zh", "zl", "x", "core")
    whole, both, turned, flat = P(fsdp, None), P(fsdp, "y"), P("y", fsdp), P(fsdp)

    return jax.shard_map(
        functools.partial(on_device, depth),
        mesh=fine,
        in_specs=(
            whole, whole, whole, flat, both, both, both, turned, P(), P(), flat, both, both, turned
        ),
        out_specs=(
            whole, whole, flat, both, both, both, turned, P(), P(), flat, both, both, turned
        ),
        check_vma=False,
    )
```

```python
import functools

import jax
import jax.numpy as jnp
from jax import lax
from jax.experimental import pallas as pl
from jax.experimental.pallas import tpu as pltpu
from jax.sharding import Mesh
from jax.sharding import PartitionSpec as P


epsilon = 1e-06
rope_base = 1000000.0
bf16 = jnp.bfloat16
f32 = jnp.float32
MESH = pl.DeviceIdType.MESH
chunk = 16
vmem_limit = 40 * 1024 * 1024

bits = {"core": 4, "x": 2, "y": 1}
orders = (("x", "y", "core"), ("y", "x", "core"))
layer = [("core", 1), ("x", 1), ("y", 1)]


def normalize(values):
    inverse = lax.rsqrt(jnp.mean(values * values, axis=-1, keepdims=True) + epsilon)
    return values * inverse, inverse


def norm_back(upstream, normed, inverse):
    return inverse * (upstream - normed * jnp.mean(upstream * normed, axis=-1, keepdims=True))


def dot(left, right):
    return jnp.dot(left, right, preferred_element_type=f32)


def dot_tn(left, right):
    return lax.dot_general(left, right, (((0,), (0,)), ((), ())), preferred_element_type=f32)


def dot_nt(left, right):
    return lax.dot_general(left, right, (((1,), (1,)), ((), ())), preferred_element_type=f32)


def parts_of(width, count):
    tiles = width // 128
    edges = [i * (tiles // count) * 128 for i in range(count)] + [width]
    return [pl.ds(edges[i], edges[i + 1] - edges[i]) for i in range(count)]


def neighbour(axis, step=1):
    return {axis: lax.axis_index(axis) ^ step}


def square_id(step):
    return {"x": lax.axis_index("x") ^ (step >> 1), "core": lax.axis_index("core") ^ (step & 1)}


def square_place(step):
    device = square_id(step)
    return device["x"] * 2 + device["core"]


square = [("core", 1), ("x", 1), ("both", 0)]


def greet(axes):
    barrier = pltpu.get_barrier_semaphore()
    for axis in axes:
        device = square_id(3) if axis[0] == "both" else neighbour(*axis)
        pl.semaphore_signal(barrier, inc=1, device_id=device, device_id_type=MESH)
    pl.semaphore_wait(barrier, len(axes))


def copy_to(device, source, target, sems, number):
    return pltpu.make_async_remote_copy(
        src_ref=source,
        dst_ref=target,
        send_sem=sems[0].at[number],
        recv_sem=sems[1].at[number],
        device_id=device,
        device_id_type=MESH,
    )


def sem_pair(count):
    return [pltpu.SemaphoreType.DMA((count,)), pltpu.SemaphoreType.DMA((count,))]


def over_rows(rows, body):
    def step(i, carry):
        body(pl.ds(pl.multiple_of(i * chunk, chunk), chunk))
        return carry

    lax.fori_loop(0, rows // chunk, step, 0)


def gather_blocks(blocks, sems):
    gather_finish(*gather_start(blocks, sems))


def gather_start(blocks, sems):
    parts = parts_of(blocks.shape[2], len(orders))
    copies = {}

    def send(p, axis, i):
        copies[p, axis, i] = copy_to(
            neighbour(axis),
            blocks.at[i, :, parts[p]],
            blocks.at[i ^ bits[axis], :, parts[p]],
            sems,
            len(copies),
        )
        copies[p, axis, i].start()

    for place in range(3):
        for p, order in enumerate(orders):
            send(p, order[place], 0)
    return copies, send


def gather_finish(copies, send):
    for p, (a, b, c) in enumerate(orders):
        copies[p, a, 0].wait_recv()
        send(p, b, bits[a])
        send(p, c, bits[a])
    for p, (a, b, c) in enumerate(orders):
        copies[p, b, 0].wait_recv()
        send(p, c, bits[b])
        copies[p, b, bits[a]].wait_recv()
        send(p, c, bits[a] ^ bits[b])
    for p, (a, b, c) in enumerate(orders):
        for i in (0, bits[a], bits[b], bits[a] ^ bits[b]):
            copies[p, c, i].wait_recv()
    for copy in copies.values():
        copy.wait_send()


class Scatter:
    def __init__(self, blocks, scratch):
        self.blocks = blocks
        self.first, self.second, self.third, self.sent = scratch[:4]
        self.sems = scratch[4:6]
        self.parts = parts_of(blocks.shape[2], len(orders))
        self.copies = []
        self.arrive = {}

    def send(self, axis, source, target):
        self.copies.append(
            copy_to(neighbour(axis), source, target, self.sems, len(self.copies))
        )
        self.copies[-1].start()
        return self.copies[-1]

    def ready(self, i):
        for p, (a, b, c) in enumerate(orders):
            if i & bits[c]:
                k = (1 if i & bits[a] else 0) + (2 if i & bits[b] else 0)
                self.arrive[p, k] = self.send(
                    c, self.blocks.at[i, :, self.parts[p]], self.first.at[k, :, self.parts[p]]
                )

    def steps(self):
        rows = self.blocks.shape[1]
        blocks, first, second, sent = self.blocks, self.first, self.second, self.sent
        for k in (3, 2):
            for p, (a, b, c) in enumerate(orders):
                j = (bits[a] if k & 1 else 0) ^ bits[b]
                part = self.parts[p]
                self.arrive[p, k].wait_recv()

                def add(row, j=j, k=k, part=part):
                    value = blocks[j, row, part].astype(f32) + first[k, row, part].astype(f32)
                    sent[k - 1, row, part] = value.astype(bf16)

                over_rows(rows, add)
                self.arrive[p, k + 2] = self.send(
                    b, sent.at[k - 1, :, part], second.at[k - 2, :, part]
                )
                yield
        for p, (a, b, c) in enumerate(orders):
            part = self.parts[p]
            self.arrive[p, 1].wait_recv()
            self.arrive[p, 5].wait_recv()

            def add(row, j=bits[a], part=part):
                value = blocks[j, row, part].astype(f32) + first[1, row, part].astype(f32)
                value = value + second[1, row, part].astype(f32)
                sent[0, row, part] = value.astype(bf16)

            over_rows(rows, add)
            self.arrive[p, 6] = self.send(a, sent.at[0, :, part], self.third.at[0, :, part])
            yield
        for p in range(len(orders)):
            for k in (0, 4, 6):
                self.arrive[p, k].wait_recv()
        for copy in self.copies:
            copy.wait_send()

    def run(self):
        for _ in self.steps():
            pass

    def row(self, row):
        value = self.blocks[0, row].astype(f32) + self.first[0, row].astype(f32)
        return value + self.second[0, row].astype(f32) + self.third[0, row].astype(f32)


block_order = (7, 6, 5, 3, 4, 2, 1, 0)


def scatter_scratch(rows, width):
    return [
        pltpu.VMEM((4, rows, width), bf16),
        pltpu.VMEM((2, rows, width), bf16),
        pltpu.VMEM((1, rows, width), bf16),
        pltpu.VMEM((3, rows, width), bf16),
        *sem_pair(7 * len(orders)),
    ]


def call(kernel, number, outputs, scratch, *operands):
    return pl.pallas_call(
        kernel,
        out_shape=outputs,
        in_specs=[pl.BlockSpec(memory_space=pltpu.VMEM)] * len(operands),
        out_specs=jax.tree.map(lambda _: pl.BlockSpec(memory_space=pltpu.VMEM), outputs),
        scratch_shapes=scratch,
        compiler_params=pltpu.CompilerParams(
            collective_id=number, has_side_effects=True, vmem_limit_bytes=vmem_limit
        ),
    )(*operands)


def start_all(copies):
    for copy in copies:
        copy.start()
    return copies


def wait_all(copies):
    for copy in copies:
        copy.wait()


def spread_start(sources, targets, sems, number=0):
    me = square_place(0)
    copies = []
    for source, (target, at) in zip(sources, targets):
        size = source.shape[1] // 4
        into = target.at[me, :, pl.ds(at, size)]

        def piece(place, source=source, size=size):
            return source.at[:, pl.ds(pl.multiple_of(place * size, size), size)]

        for step in (3, 1, 2):
            away = piece(square_place(step))
            copies.append(copy_to(square_id(step), away, into, sems, number + step))
        copies.append(pltpu.make_async_copy(piece(me), into, sems[0].at[number]))
        number += 4
    return start_all(copies)


def collect_start(sources, targets, sems):
    me = square_place(0)
    copies = []
    for number, ((source, at), target) in enumerate(zip(sources, targets)):
        size = target.shape[1] // 4
        into = target.at[:, pl.ds(pl.multiple_of(me * size, size), size)]
        for step in (3, 1, 2):
            away = source.at[square_place(step), :, pl.ds(at, size)]
            copies.append(copy_to(square_id(step), away, into, sems, number * 4 + step))
        copies.append(
            pltpu.make_async_copy(source.at[me, :, pl.ds(at, size)], into, sems[0].at[number * 4])
        )
    return start_all(copies)


def enter_kernel(query, key, value, output, segments, slabs, segments_all, *sems):
    greet(square)
    size, other = query.shape[1] // 4, key.shape[1] // 4
    targets = [(slabs, at) for at in (0, size, size + other, size + 2 * other)]
    copies = spread_start((query, key, value, output), targets, sems[:2])
    segments_all[0] = segments[...]
    copies += start_all(
        [
            copy_to(
                square_id(step),
                segments,
                segments_all.at[step // 2 + step % 2 * 2],
                sems[2:],
                step,
            )
            for step in (1, 2, 3)
        ]
    )
    wait_all(copies)


def tokens_kernel(tokens, gate, up, down, inputs_all, gate_up_slabs, down_slabs, *sems):
    greet(square + [("y", 1)])

    def norm(row):
        normed, _ = normalize(tokens[row].astype(f32))
        inputs_all[0, row] = normed.astype(bf16)

    over_rows(tokens.shape[0], norm)
    hidden = gate.shape[1] // 4
    targets = ((gate_up_slabs, 0), (gate_up_slabs, hidden), (down_slabs, 0))
    gather = gather_start(inputs_all, sems[:2])
    copies = spread_start((gate, up, down), targets, sems[2:])
    gather_finish(*gather)
    wait_all(copies)


def grads_kernel(grads, grads_all, *sems):
    greet(layer)
    grads_all[0] = grads[...]
    gather_blocks(grads_all, sems)


def turn(value, cosine, sine):
    return value * cosine + pltpu.roll(value, value.shape[1] // 2, 1) * sine


def allowed_of(start):
    rows = lax.broadcasted_iota(jnp.int32, start.shape, 0)
    columns = lax.broadcasted_iota(jnp.int32, start.shape, 1)
    return (columns >= start) & (columns <= rows)


def probabilities(queries, keys, allowed):
    scores = dot_nt(queries, keys) * queries.shape[1] ** (-0.5)
    scores = jnp.where(allowed, scores, -1e30)
    powers = jnp.exp(scores - jnp.max(scores, axis=1, keepdims=True))
    return powers / jnp.sum(powers, axis=1, keepdims=True)


def head_columns(heads, groups, size):
    query = [pl.ds(h * size, size) for h in range(heads)]
    key = [pl.ds((heads + g) * size, size) for g in range(groups)]
    value = [pl.ds((heads + groups + g) * size, size) for g in range(groups)]
    return query, key, value


def middle_kernel(counts, qkv, cosine, sine, start, gains, output, tokens, attended,
                  residual, inputs_all, partial, *scratch):
    greet(layer)
    heads, groups, size = counts
    rows = tokens.shape[0]
    query, key, value = head_columns(heads, groups, size)
    total = Scatter(partial, scratch[:6])
    for i in block_order:
        row = pl.ds(i * rows, rows)
        cos, sin = cosine[row], sine[row]
        allowed = allowed_of(start[row])
        for g in range(groups):
            keys = turn(normalize(qkv[row, key[g]])[0] * gains[1:2], cos, sin).astype(bf16)
            values = qkv[row, value[g]].astype(bf16)
            for h in range(g * (heads // groups), (g + 1) * (heads // groups)):
                queries = normalize(qkv[row, query[h]])[0] * gains[0:1]
                queries = turn(queries, cos, sin).astype(bf16)
                probs = probabilities(queries, keys, allowed)
                attended[row, query[h]] = dot(probs.astype(bf16), values).astype(bf16)
        product = output[:, pl.ds(output.shape[1] - heads * size, heads * size)]
        partial[i] = dot_nt(attended[row], product).astype(bf16)
        total.ready(i)
    total.run()

    def norm(row):
        value = total.row(row) + tokens[row].astype(f32)
        residual[row] = value
        inputs_all[0, row] = normalize(value)[0].astype(bf16)

    over_rows(rows, norm)
    gather_blocks(inputs_all, scratch[6:8])


def back_kernel(partial, residual, grads, d_residual, low_all, *scratch):
    greet(layer)
    total = Scatter(partial, scratch[:6])
    for i in block_order:
        total.ready(i)
    total.run()

    def norm(row):
        normed, inverse = normalize(residual[row])
        value = grads[row].astype(f32) + norm_back(total.row(row), normed, inverse)
        d_residual[row] = value
        low_all[0, row] = value.astype(bf16)

    over_rows(residual.shape[0], norm)
    gather_blocks(low_all, scratch[6:8])


def share_start(own, both, sems):
    mine = lax.axis_index("y")
    return start_all(
        [
            copy_to(neighbour("y"), own, both.at[mine], sems, 0),
            pltpu.make_async_copy(own, both.at[mine], sems[0].at[1]),
        ]
    )


def heads_kernel(counts, rows, qkv, cosine, sine, start, gains, d_attended, d_qkv, gain_sums):
    heads, groups, size = counts
    scale = size ** (-0.5)
    query, key, value = head_columns(heads, groups, size)
    query_sum = jnp.zeros((1, size), f32)
    key_sum = jnp.zeros((1, size), f32)
    for i in range(8):
        row = pl.ds(i * rows, rows)
        cos, sin = cosine[row], sine[row]
        allowed = allowed_of(start[row])
        for g in range(groups):
            key_hat, key_inverse = normalize(qkv[row, key[g]])
            keys = turn(key_hat * gains[1:2], cos, sin).astype(bf16)
            values = qkv[row, value[g]].astype(bf16)
            d_keys = d_values = 0.0
            for h in range(g * (heads // groups), (g + 1) * (heads // groups)):
                query_hat, query_inverse = normalize(qkv[row, query[h]])
                queries = turn(query_hat * gains[0:1], cos, sin).astype(bf16)
                probs = probabilities(queries, keys, allowed)
                upstream = d_attended[row, query[h]]
                d_values = d_values + dot_tn(probs.astype(bf16), upstream)
                d_probs = dot_nt(upstream, values)
                inner = jnp.sum(d_probs * probs, axis=1, keepdims=True)
                d_scores = (probs * (d_probs - inner)).astype(bf16)
                d_keys = d_keys + dot_tn(d_scores, queries)
                d_query = turn(dot(d_scores, keys) * scale, cos, -sin)
                query_sum = query_sum + jnp.sum(d_query * query_hat, axis=0, keepdims=True)
                d_qkv[row, query[h]] = norm_back(
                    d_query * gains[0:1], query_hat, query_inverse
                ).astype(bf16)
            d_key = turn(d_keys * scale, cos, -sin)
            key_sum = key_sum + jnp.sum(d_key * key_hat, axis=0, keepdims=True)
            d_qkv[row, key[g]] = norm_back(d_key * gains[1:2], key_hat, key_inverse).astype(bf16)
            d_qkv[row, value[g]] = d_values.astype(bf16)
    gain_sums[0:1] = query_sum
    gain_sums[1:2] = key_sum


def leave_kernel(depth, partial, mixed_partial, tokens, residual, d_residual,
                 gain_sums, grad_tokens, mixed_own, gain_totals, token_grads, *scratch):
    stages = layer + [("z", 1 << n) for n in range(depth.bit_length() - 1)]
    greet(stages)
    total = Scatter(partial, scratch[:6])
    other = Scatter(mixed_partial, scratch[6:12])
    for scatter in (total, other):
        for i in block_order:
            scatter.ready(i)
    held, arrived, sems = scratch[12], scratch[13], scratch[14:16]
    held[0] = gain_sums[...]
    ticks = total.steps()
    for n, axis in enumerate(stages):
        copy = copy_to(neighbour(*axis), held.at[n], arrived.at[n], sems, n)
        copy.start()
        next(ticks, None)
        copy.wait()
        held[n + 1] = held[n] + arrived[n]
    gain_totals[...] = held[len(stages)]
    other_ticks = other.steps()
    for _ in ticks:
        next(other_ticks, None)

    def norm(row):
        normed, inverse = normalize(tokens[row].astype(f32))
        value = d_residual[row] + norm_back(total.row(row), normed, inverse)
        token_grads[row] = value.astype(bf16)

    over_rows(tokens.shape[0], norm)
    shared = share_start(token_grads, grad_tokens, scratch[16:18])
    for _ in other_ticks:
        pass

    def add(row):
        mixed_own[row] = (residual[row] + other.row(row)).astype(bf16)

    over_rows(tokens.shape[0], add)
    wait_all(shared)


def gate_up_kernel(slabs, down_slabs, mixed_own, grad_gate, grad_up, grad_down, mixed, *sems):
    greet(square + [("y", 1)])
    shared = share_start(mixed_own, mixed, sems[2:])
    sources = ((slabs, 0), (slabs, grad_gate.shape[1] // 4), (down_slabs, 0))
    wait_all(collect_start(sources, (grad_gate, grad_up, grad_down), sems[:2]))
    wait_all(shared)


def collect_kernel(slabs, grad_query, grad_key, grad_value, grad_output, *sems):
    greet(square)
    size, other = grad_query.shape[1] // 4, grad_key.shape[1] // 4
    sources = ((slabs, 0), (slabs, size), (slabs, size + other), (slabs, size + 2 * other))
    targets = (grad_query, grad_key, grad_value, grad_output)
    wait_all(collect_start(sources, targets, sems))


def tables(segments, size):
    rows = segments.shape[1]
    index_row = jnp.arange(rows)
    same_seg = segments[:, :, None] == segments[:, None, :]
    earlier = index_row[:, None] > index_row[None, :]
    position = jnp.sum(jnp.where(same_seg & earlier, 1, 0), axis=-1)
    frequency = rope_base ** (-2.0 * jnp.arange(size // 2).astype(f32) / size)
    angles = (position.astype(f32)[:, :, None] * frequency).reshape(-1, size // 2)
    cosine, sine = jnp.cos(angles), jnp.sin(angles)
    first = (index_row - position).reshape(-1, 1)
    return (
        jnp.concatenate([cosine, cosine], axis=1),
        jnp.concatenate([-sine, sine], axis=1),
        jnp.broadcast_to(first, (first.shape[0], rows)).astype(jnp.int32),
    )


def swap(values, axis):
    return lax.ppermute(values, axis, [(0, 1), (1, 0)])


def fetch(spread):
    columns = spread.shape[2]
    return lax.all_gather(spread.reshape(-1, columns), "z", axis=0, tiled=True)


def give_back(grads):
    summed_rows = lax.psum_scatter(grads, "z", scatter_dimension=0, tiled=True)
    return summed_rows.reshape(4, -1, grads.shape[1])


def on_device(depth, tokens, grad_out, segments, attention_gain, query_weight, key_weight,
              value_weight, output_weight, query_gain, key_gain, feedforward_gain, gate_weight,
              up_weight, down_weight):
    size = query_gain.shape[0]
    blocks, rows = segments.shape
    width = tokens.shape[1]
    rows_here = attention_gain.shape[0]
    heads = query_weight.shape[1] // size // 4
    groups = key_weight.shape[1] // size // 4
    counts = (heads, groups, size)
    mine = lax.axis_index("y")
    gain_one, gain_two = attention_gain[:, None], feedforward_gain[:, None]

    def array(dtype, *dims):
        return jax.ShapeDtypeStruct(dims, dtype)

    def scaled(weight, gain):
        return (weight.astype(f32) * gain).astype(bf16)

    def own(values):
        return lax.dynamic_index_in_dim(
            values.reshape(2, -1, values.shape[-1]), mine, 0, keepdims=False
        )

    token_own, grad_own = own(tokens), own(grad_out)
    block_rows = token_own.shape[0]
    block = array(f32, block_rows, width)
    both = array(bf16, 2, block_rows, width)
    everyone = array(bf16, 8, block_rows, width)
    qkv_size = (heads + 2 * groups) * size
    output_size = heads * size
    hidden_size = gate_weight.shape[1] // 4

    def scatter_shapes():
        return scatter_scratch(block_rows, width)

    pairs = segments.reshape(2, -1, rows)
    pairs = jnp.where(mine == 0, pairs, pairs[::-1]).reshape(blocks, rows)
    attention_slabs, segments_all = call(
        enter_kernel,
        1,
        (array(bf16, 4, rows_here, qkv_size + output_size), array(jnp.int32, 4, blocks, rows)),
        sem_pair(16) + sem_pair(4),
        *(scaled(w, gain_one) for w in (query_weight, key_weight, value_weight)),
        output_weight.T,
        pairs,
    )
    attention_all = fetch(attention_slabs)
    qkv_weight = attention_all[:, :qkv_size]
    token_own, _ = lax.optimization_barrier((token_own, segments_all))
    input_one, gate_up_slabs, down_slabs = call(
        tokens_kernel,
        2,
        (
            everyone,
            array(bf16, 4, rows_here, 2 * hidden_size),
            array(bf16, 4, rows_here, hidden_size),
        ),
        sem_pair(14) + sem_pair(12),
        token_own,
        scaled(gate_weight, gain_two),
        scaled(up_weight, gain_two),
        down_weight.T,
    )
    input_one = input_one.reshape(-1, width)
    gate_up_all = fetch(gate_up_slabs)
    down_all = fetch(down_slabs)
    cosine, sine, start = tables(segments_all.reshape(-1, rows), size)
    gains = jnp.stack([query_gain, key_gain])

    qkv = dot(input_one, qkv_weight)
    attended, residual, input_two = call(
        functools.partial(middle_kernel, counts),
        3,
        (array(bf16, 8 * block_rows, output_size), block, everyone),
        [pltpu.VMEM((8, block_rows, width), bf16)] + scatter_shapes() + sem_pair(14),
        qkv,
        cosine,
        sine,
        start,
        gains,
        attention_all,
        token_own,
    )
    input_two = input_two.reshape(-1, width)
    grad_own, _ = lax.optimization_barrier((grad_own, residual))
    grads_all = call(grads_kernel, 4, everyone, sem_pair(14), grad_own).reshape(-1, width)

    gate_up = dot(input_two, gate_up_all)
    gate_pre, up_pre = gate_up[:, :hidden_size], gate_up[:, hidden_size:]
    sigma = jax.nn.sigmoid(gate_pre)
    hidden = (gate_pre * sigma * up_pre).astype(bf16)
    grad_down = dot_tn(grads_all, hidden).astype(bf16)
    _, hidden, gate_pre, up_pre, down_all = lax.optimization_barrier(
        (grad_down, hidden, gate_pre, up_pre, down_all)
    )
    sigma = jax.nn.sigmoid(gate_pre)
    grad_down = give_back(grad_down)
    d_hidden = dot(grads_all, down_all)
    d_gate = (d_hidden * up_pre * sigma * (1.0 + gate_pre * (1.0 - sigma))).astype(bf16)
    d_up = (d_hidden * gate_pre * sigma).astype(bf16)
    d_gate_up = jnp.concatenate([d_gate, d_up], axis=1)
    grad_gate_up = dot_tn(input_two, d_gate_up).astype(bf16)
    partial = dot_nt(d_gate_up, gate_up_all).astype(bf16).reshape(8, -1, width)
    grad_gate_up, partial = lax.optimization_barrier((grad_gate_up, partial))
    d_residual, d_residual_low = call(
        back_kernel,
        5,
        (block, everyone),
        scatter_shapes() + sem_pair(14),
        partial,
        residual,
        grad_own,
    )
    d_residual_low = d_residual_low.reshape(-1, width)
    grad_gate_up = give_back(grad_gate_up)

    grad_output = dot_tn(d_residual_low, attended).astype(bf16)
    d_attended = dot(d_residual_low, attention_all[:, qkv_size:]).astype(bf16)
    d_qkv, gain_sums = pl.pallas_call(
        functools.partial(heads_kernel, counts, block_rows),
        out_shape=(array(bf16, 8 * block_rows, qkv_size), array(f32, 2, size)),
        in_specs=[pl.BlockSpec(memory_space=pltpu.VMEM)] * 6,
        out_specs=(pl.BlockSpec(memory_space=pltpu.VMEM),) * 2,
        compiler_params=pltpu.CompilerParams(vmem_limit_bytes=vmem_limit),
        name="heads",
    )(qkv, cosine, sine, start, gains, d_attended)
    grad_attention = jnp.concatenate(
        [dot_tn(input_one, d_qkv).astype(bf16), grad_output], axis=1
    )
    late, d_last, grad_attention = lax.optimization_barrier((hidden, d_qkv, grad_attention))
    partial = dot_nt(d_last, qkv_weight).astype(bf16).reshape(8, -1, width)
    mixed_partial = dot_nt(late, down_all).astype(bf16).reshape(8, -1, width)
    grad_attention = give_back(grad_attention)
    stages = 3 + depth.bit_length() - 1
    grad_tokens, mixed_own, head_gains = call(
        functools.partial(leave_kernel, depth),
        7,
        (
            both,
            array(bf16, block_rows, width),
            array(f32, 2, size),
        ),
        [pltpu.VMEM((block_rows, width), bf16)]
        + scatter_shapes()
        + scatter_shapes()
        + [pltpu.VMEM((stages + 1, 2, size), f32), pltpu.VMEM((stages, 2, size), f32)]
        + sem_pair(stages)
        + sem_pair(2),
        partial,
        mixed_partial,
        token_own,
        residual,
        d_residual,
        gain_sums,
    )
    raw_gate, raw_up, raw_down, mixed = call(
        gate_up_kernel,
        8,
        (*(array(bf16, rows_here, 4 * hidden_size) for _ in range(3)), both),
        sem_pair(12) + sem_pair(2),
        grad_gate_up,
        grad_down,
        mixed_own,
    )
    grad_attention, _ = lax.optimization_barrier((grad_attention, mixed))
    raw_query, raw_key, raw_value, raw_output = call(
        collect_kernel,
        9,
        (
            array(bf16, *query_weight.shape),
            array(bf16, *key_weight.shape),
            array(bf16, *value_weight.shape),
            array(bf16, rows_here, 4 * output_size),
        ),
        sem_pair(16),
        grad_attention,
    )

    def finish(raw, weights, gain):
        raw = [g.astype(f32) for g in raw]
        sums = sum(jnp.sum(w.astype(f32) * g, axis=1) for w, g in zip(weights, raw))
        sums = sums.reshape(1, rows_here)
        return [g * gain for g in raw], (sums + swap(sums, "y"))[0]

    (grad_query, grad_key, grad_value), grad_one = finish(
        (raw_query, raw_key, raw_value), (query_weight, key_weight, value_weight), gain_one
    )
    (grad_gate, grad_up), grad_two = finish((raw_gate, raw_up), (gate_weight, up_weight), gain_two)
    return (
        mixed.reshape(-1, width),
        grad_tokens.reshape(-1, width).astype(f32),
        grad_one,
        grad_query,
        grad_key,
        grad_value,
        raw_output.T.astype(f32),
        head_gains[0],
        head_gains[1],
        grad_two,
        grad_gate,
        grad_up,
        raw_down.T.astype(f32),
    )


def solution(mesh):
    depth = mesh.shape["fsdp"] // 4
    fine = Mesh(
        mesh.devices.reshape(depth, 2, 2, mesh.shape["tensor"]), ("z", "x", "core", "y")
    )
    fsdp = ("z", "x", "core")
    whole, both, turned, flat = P(fsdp, None), P(fsdp, "y"), P("y", fsdp), P(fsdp)

    def step(*arrays):
        return on_device(depth, *arrays)

    return jax.shard_map(
        step,
        mesh=fine,
        in_specs=(
            whole, whole, whole, flat, both, both, both, turned, P(), P(), flat, both, both, turned
        ),
        out_specs=(
            whole, whole, flat, both, both, both, turned, P(), P(), flat, both, both, turned
        ),
        check_vma=False,
    )
```

```python
import functools

import jax
import jax.numpy as jnp
from jax import lax
from jax.experimental import pallas as pl
from jax.experimental.pallas import tpu as pltpu
from jax.sharding import Mesh
from jax.sharding import PartitionSpec as P


epsilon = 1e-06
rope_base = 1000000.0
bf16 = jnp.bfloat16
f32 = jnp.float32
MESH = pl.DeviceIdType.MESH
chunk = 16
vmem_limit = 40 * 1024 * 1024

bits = {"core": 4, "x": 2, "y": 1}
orders = (("x", "y", "core"), ("y", "x", "core"))
layer = [("core", 1), ("x", 1), ("y", 1)]


def normalize(values):
    inverse = lax.rsqrt(jnp.mean(values * values, axis=-1, keepdims=True) + epsilon)
    return values * inverse, inverse


def norm_back(upstream, normed, inverse):
    return inverse * (upstream - normed * jnp.mean(upstream * normed, axis=-1, keepdims=True))


def dot(left, right):
    return jnp.dot(left, right, preferred_element_type=f32)


def dot_tn(left, right):
    return lax.dot_general(left, right, (((0,), (0,)), ((), ())), preferred_element_type=f32)


def dot_nt(left, right):
    return lax.dot_general(left, right, (((1,), (1,)), ((), ())), preferred_element_type=f32)


def parts_of(width, count):
    tiles = width // 128
    edges = [i * (tiles // count) * 128 for i in range(count)] + [width]
    return [pl.ds(edges[i], edges[i + 1] - edges[i]) for i in range(count)]


def neighbour(axis, step=1):
    return {axis: lax.axis_index(axis) ^ step}


def square_id(step):
    return {"x": lax.axis_index("x") ^ (step >> 1), "core": lax.axis_index("core") ^ (step & 1)}


def square_place(step):
    device = square_id(step)
    return device["x"] * 2 + device["core"]


square = [("core", 1), ("x", 1), ("both", 0)]


def greet(axes):
    barrier = pltpu.get_barrier_semaphore()
    for axis in axes:
        device = square_id(3) if axis[0] == "both" else neighbour(*axis)
        pl.semaphore_signal(barrier, inc=1, device_id=device, device_id_type=MESH)
    pl.semaphore_wait(barrier, len(axes))


def copy_to(device, source, target, sems, number):
    return pltpu.make_async_remote_copy(
        src_ref=source,
        dst_ref=target,
        send_sem=sems[0].at[number],
        recv_sem=sems[1].at[number],
        device_id=device,
        device_id_type=MESH,
    )


def sem_pair(count):
    return [pltpu.SemaphoreType.DMA((count,)), pltpu.SemaphoreType.DMA((count,))]


def over_rows(rows, body):
    def step(i, carry):
        body(pl.ds(pl.multiple_of(i * chunk, chunk), chunk))
        return carry

    lax.fori_loop(0, rows // chunk, step, 0)


def gather_blocks(blocks, sems):
    gather_finish(*gather_start(blocks, sems))


def gather_start(blocks, sems):
    parts = parts_of(blocks.shape[2], len(orders))
    copies = {}

    def send(p, axis, i):
        copies[p, axis, i] = copy_to(
            neighbour(axis),
            blocks.at[i, :, parts[p]],
            blocks.at[i ^ bits[axis], :, parts[p]],
            sems,
            len(copies),
        )
        copies[p, axis, i].start()

    for place in range(3):
        for p, order in enumerate(orders):
            send(p, order[place], 0)
    return copies, send


def gather_finish(copies, send):
    for p, (a, b, c) in enumerate(orders):
        copies[p, a, 0].wait_recv()
        send(p, b, bits[a])
        send(p, c, bits[a])
    for p, (a, b, c) in enumerate(orders):
        copies[p, b, 0].wait_recv()
        send(p, c, bits[b])
        copies[p, b, bits[a]].wait_recv()
        send(p, c, bits[a] ^ bits[b])
    for p, (a, b, c) in enumerate(orders):
        for i in (0, bits[a], bits[b], bits[a] ^ bits[b]):
            copies[p, c, i].wait_recv()
    for copy in copies.values():
        copy.wait_send()


class Scatter:
    def __init__(self, blocks, scratch):
        self.blocks = blocks
        self.first, self.second, self.third, self.sent = scratch[:4]
        self.sems = scratch[4:6]
        self.parts = parts_of(blocks.shape[2], len(orders))
        self.copies = []
        self.arrive = {}

    def send(self, axis, source, target):
        self.copies.append(
            copy_to(neighbour(axis), source, target, self.sems, len(self.copies))
        )
        self.copies[-1].start()
        return self.copies[-1]

    def ready(self, i):
        for p, (a, b, c) in enumerate(orders):
            if i & bits[c]:
                k = (1 if i & bits[a] else 0) + (2 if i & bits[b] else 0)
                self.arrive[p, k] = self.send(
                    c, self.blocks.at[i, :, self.parts[p]], self.first.at[k, :, self.parts[p]]
                )

    def steps(self):
        rows = self.blocks.shape[1]
        blocks, first, second, sent = self.blocks, self.first, self.second, self.sent
        for k in (3, 2):
            for p, (a, b, c) in enumerate(orders):
                j = (bits[a] if k & 1 else 0) ^ bits[b]
                part = self.parts[p]
                self.arrive[p, k].wait_recv()

                def add(row, j=j, k=k, part=part):
                    value = blocks[j, row, part].astype(f32) + first[k, row, part].astype(f32)
                    sent[k - 1, row, part] = value.astype(bf16)

                over_rows(rows, add)
                self.arrive[p, k + 2] = self.send(
                    b, sent.at[k - 1, :, part], second.at[k - 2, :, part]
                )
                yield
        for p, (a, b, c) in enumerate(orders):
            part = self.parts[p]
            self.arrive[p, 1].wait_recv()
            self.arrive[p, 5].wait_recv()

            def add(row, j=bits[a], part=part):
                value = blocks[j, row, part].astype(f32) + first[1, row, part].astype(f32)
                value = value + second[1, row, part].astype(f32)
                sent[0, row, part] = value.astype(bf16)

            over_rows(rows, add)
            self.arrive[p, 6] = self.send(a, sent.at[0, :, part], self.third.at[0, :, part])
            yield
        for p in range(len(orders)):
            for k in (0, 4, 6):
                self.arrive[p, k].wait_recv()
        for copy in self.copies:
            copy.wait_send()

    def run(self):
        for _ in self.steps():
            pass

    def row(self, row):
        value = self.blocks[0, row].astype(f32) + self.first[0, row].astype(f32)
        return value + self.second[0, row].astype(f32) + self.third[0, row].astype(f32)


def products(scatter, left, right, columns):
    rows = scatter.blocks.shape[1]

    def step(i, carry):
        row = pl.ds(pl.multiple_of(i * rows, rows), rows)
        scatter.blocks[i] = dot_nt(left[row], right[:, columns]).astype(bf16)
        return carry

    lax.fori_loop(0, 8, step, 0)
    for i in range(4, 8):
        scatter.ready(i)


def scatter_scratch(rows, width):
    return [
        pltpu.VMEM((4, rows, width), bf16),
        pltpu.VMEM((2, rows, width), bf16),
        pltpu.VMEM((1, rows, width), bf16),
        pltpu.VMEM((3, rows, width), bf16),
        *sem_pair(7 * len(orders)),
    ]


def call(kernel, number, outputs, scratch, *operands):
    return pl.pallas_call(
        kernel,
        out_shape=outputs,
        in_specs=[pl.BlockSpec(memory_space=pltpu.VMEM)] * len(operands),
        out_specs=jax.tree.map(lambda _: pl.BlockSpec(memory_space=pltpu.VMEM), outputs),
        scratch_shapes=scratch,
        compiler_params=pltpu.CompilerParams(
            collective_id=number, has_side_effects=True, vmem_limit_bytes=vmem_limit
        ),
    )(*operands)


def start_all(copies):
    for copy in copies:
        copy.start()
    return copies


def wait_all(copies):
    for copy in copies:
        copy.wait()


def spread_start(sources, targets, sems, number=0):
    me = square_place(0)
    copies = []
    for source, (target, at) in zip(sources, targets):
        size = source.shape[1] // 4
        into = target.at[me, :, pl.ds(at, size)]

        def piece(place, source=source, size=size):
            return source.at[:, pl.ds(pl.multiple_of(place * size, size), size)]

        for step in (3, 1, 2):
            away = piece(square_place(step))
            copies.append(copy_to(square_id(step), away, into, sems, number + step))
        copies.append(pltpu.make_async_copy(piece(me), into, sems[0].at[number]))
        number += 4
    return start_all(copies)


def collect_start(sources, targets, sems):
    me = square_place(0)
    copies = []
    for number, ((source, at), target) in enumerate(zip(sources, targets)):
        size = target.shape[1] // 4
        into = target.at[:, pl.ds(pl.multiple_of(me * size, size), size)]
        for step in (3, 1, 2):
            away = source.at[square_place(step), :, pl.ds(at, size)]
            copies.append(copy_to(square_id(step), away, into, sems, number * 4 + step))
        copies.append(
            pltpu.make_async_copy(source.at[me, :, pl.ds(at, size)], into, sems[0].at[number * 4])
        )
    return start_all(copies)


def enter_kernel(query, key, value, output, segments, slabs, segments_all, *sems):
    greet(square)
    size, other = query.shape[1] // 4, key.shape[1] // 4
    targets = [(slabs, at) for at in (0, size, size + other, size + 2 * other)]
    copies = spread_start((query, key, value, output), targets, sems[:2])
    segments_all[0] = segments[...]
    copies += start_all(
        [
            copy_to(
                square_id(step),
                segments,
                segments_all.at[step // 2 + step % 2 * 2],
                sems[2:],
                step,
            )
            for step in (1, 2, 3)
        ]
    )
    wait_all(copies)


def tokens_kernel(tokens, gate, up, down, inputs_all, gate_up_slabs, down_slabs, *sems):
    greet(square + [("y", 1)])

    def norm(row):
        normed, _ = normalize(tokens[row].astype(f32))
        inputs_all[0, row] = normed.astype(bf16)

    over_rows(tokens.shape[0], norm)
    hidden = gate.shape[1] // 4
    targets = ((gate_up_slabs, 0), (gate_up_slabs, hidden), (down_slabs, 0))
    gather = gather_start(inputs_all, sems[:2])
    copies = spread_start((gate, up, down), targets, sems[2:])
    gather_finish(*gather)
    wait_all(copies)


def grads_kernel(grads, grads_all, *sems):
    greet(layer)
    grads_all[0] = grads[...]
    gather_blocks(grads_all, sems)


def turn(value, cosine, sine):
    return value * cosine + pltpu.roll(value, value.shape[1] // 2, 1) * sine


def block_tables(start, cosine, sine):
    rows = lax.broadcasted_iota(jnp.int32, start.shape, 0)
    columns = lax.broadcasted_iota(jnp.int32, start.shape, 1)
    pick = jnp.where(columns == rows - start, 1.0, 0.0)
    cos, sin = (
        jnp.dot(pick, table[...], precision=lax.Precision.HIGHEST, preferred_element_type=f32)
        for table in (cosine, sine)
    )
    return (columns >= start) & (columns <= rows), cos, sin


def probabilities(queries, keys, allowed):
    scores = dot_nt(queries, keys) * queries.shape[1] ** (-0.5)
    scores = jnp.where(allowed, scores, -1e30)
    powers = jnp.exp(scores - jnp.max(scores, axis=1, keepdims=True))
    return powers / jnp.sum(powers, axis=1, keepdims=True)


def head_columns(heads, groups, size):
    query = [pl.ds(h * size, size) for h in range(heads)]
    key = [pl.ds((heads + g) * size, size) for g in range(groups)]
    value = [pl.ds((heads + groups + g) * size, size) for g in range(groups)]
    return query, key, value


def middle_kernel(counts, qkv, cosine, sine, start, gains, output, tokens, attended,
                  residual, inputs_all, partial, *scratch):
    greet(layer)
    heads, groups, size = counts
    rows = tokens.shape[0]
    query, key, value = head_columns(heads, groups, size)
    total = Scatter(partial, scratch[:6])

    def attend(i, carry):
        row = pl.ds(pl.multiple_of(i * rows, rows), rows)
        allowed, cos, sin = block_tables(start[row], cosine, sine)
        for g in range(groups):
            keys = turn(normalize(qkv[row, key[g]])[0] * gains[1:2], cos, sin).astype(bf16)
            values = qkv[row, value[g]].astype(bf16)
            for h in range(g * (heads // groups), (g + 1) * (heads // groups)):
                queries = normalize(qkv[row, query[h]])[0] * gains[0:1]
                queries = turn(queries, cos, sin).astype(bf16)
                probs = probabilities(queries, keys, allowed)
                attended[row, query[h]] = dot(probs.astype(bf16), values).astype(bf16)
        return carry

    lax.fori_loop(0, 8, attend, 0)
    products(total, attended, output, pl.ds(output.shape[1] - heads * size, heads * size))
    total.run()

    def norm(row):
        value = total.row(row) + tokens[row].astype(f32)
        residual[row] = value
        inputs_all[0, row] = normalize(value)[0].astype(bf16)

    over_rows(rows, norm)
    gather_blocks(inputs_all, scratch[6:8])


def back_kernel(d_gate_up, gate_up, residual, grads, d_residual, low_all, partial, *scratch):
    greet(layer)
    total = Scatter(partial, scratch[:6])
    products(total, d_gate_up, gate_up, slice(None))
    total.run()

    def norm(row):
        normed, inverse = normalize(residual[row])
        value = grads[row].astype(f32) + norm_back(total.row(row), normed, inverse)
        d_residual[row] = value
        low_all[0, row] = value.astype(bf16)

    over_rows(residual.shape[0], norm)
    gather_blocks(low_all, scratch[6:8])


def share_start(own, both, sems):
    mine = lax.axis_index("y")
    return start_all(
        [
            copy_to(neighbour("y"), own, both.at[mine], sems, 0),
            pltpu.make_async_copy(own, both.at[mine], sems[0].at[1]),
        ]
    )


def heads_kernel(counts, rows, qkv, cosine, sine, start, gains, d_attended, d_qkv, gain_sums):
    heads, groups, size = counts
    scale = size ** (-0.5)
    query, key, value = head_columns(heads, groups, size)

    def block(i, sums):
        query_sum, key_sum = sums
        row = pl.ds(pl.multiple_of(i * rows, rows), rows)
        allowed, cos, sin = block_tables(start[row], cosine, sine)
        for g in range(groups):
            key_hat, key_inverse = normalize(qkv[row, key[g]])
            keys = turn(key_hat * gains[1:2], cos, sin).astype(bf16)
            values = qkv[row, value[g]].astype(bf16)
            d_keys = d_values = 0.0
            for h in range(g * (heads // groups), (g + 1) * (heads // groups)):
                query_hat, query_inverse = normalize(qkv[row, query[h]])
                queries = turn(query_hat * gains[0:1], cos, sin).astype(bf16)
                probs = probabilities(queries, keys, allowed)
                upstream = d_attended[row, query[h]]
                d_values = d_values + dot_tn(probs.astype(bf16), upstream)
                d_probs = dot_nt(upstream, values)
                inner = jnp.sum(d_probs * probs, axis=1, keepdims=True)
                d_scores = (probs * (d_probs - inner)).astype(bf16)
                d_keys = d_keys + dot_tn(d_scores, queries)
                d_query = turn(dot(d_scores, keys) * scale, cos, -sin)
                query_sum = query_sum + jnp.sum(d_query * query_hat, axis=0, keepdims=True)
                d_qkv[row, query[h]] = norm_back(
                    d_query * gains[0:1], query_hat, query_inverse
                ).astype(bf16)
            d_key = turn(d_keys * scale, cos, -sin)
            key_sum = key_sum + jnp.sum(d_key * key_hat, axis=0, keepdims=True)
            d_qkv[row, key[g]] = norm_back(d_key * gains[1:2], key_hat, key_inverse).astype(bf16)
            d_qkv[row, value[g]] = d_values.astype(bf16)
        return query_sum, key_sum

    zeros = jnp.zeros((1, size), f32)
    query_sum, key_sum = lax.fori_loop(0, 8, block, (zeros, zeros))
    gain_sums[0:1] = query_sum
    gain_sums[1:2] = key_sum


def leave_kernel(depth, d_qkv, weights, hidden, down, tokens, residual, d_residual, gain_sums,
                 grad_tokens, mixed_own, gain_totals, partial, mixed_partial, token_grads, *scratch):
    stages = layer + [("z", 1 << n) for n in range(depth.bit_length() - 1)]
    greet(stages)
    total = Scatter(partial, scratch[:6])
    other = Scatter(mixed_partial, scratch[6:12])
    products(total, d_qkv, weights, pl.ds(0, d_qkv.shape[1]))
    products(other, hidden, down, slice(None))
    held, arrived, sems = scratch[12], scratch[13], scratch[14:16]
    held[0] = gain_sums[...]
    ticks = total.steps()
    for n, axis in enumerate(stages):
        copy = copy_to(neighbour(*axis), held.at[n], arrived.at[n], sems, n)
        copy.start()
        next(ticks, None)
        copy.wait()
        held[n + 1] = held[n] + arrived[n]
    gain_totals[...] = held[len(stages)]
    other_ticks = other.steps()
    for _ in ticks:
        next(other_ticks, None)

    def norm(row):
        normed, inverse = normalize(tokens[row].astype(f32))
        value = d_residual[row] + norm_back(total.row(row), normed, inverse)
        token_grads[row] = value.astype(bf16)

    over_rows(tokens.shape[0], norm)
    shared = share_start(token_grads, grad_tokens, scratch[16:18])
    for _ in other_ticks:
        pass

    def add(row):
        mixed_own[row] = (residual[row] + other.row(row)).astype(bf16)

    over_rows(tokens.shape[0], add)
    wait_all(shared)


def gate_up_kernel(slabs, down_slabs, mixed_own, grad_gate, grad_up, grad_down, mixed, *sems):
    greet(square + [("y", 1)])
    shared = share_start(mixed_own, mixed, sems[2:])
    sources = ((slabs, 0), (slabs, grad_gate.shape[1] // 4), (down_slabs, 0))
    wait_all(collect_start(sources, (grad_gate, grad_up, grad_down), sems[:2]))
    wait_all(shared)


def collect_kernel(slabs, grad_query, grad_key, grad_value, grad_output, *sems):
    greet(square)
    size, other = grad_query.shape[1] // 4, grad_key.shape[1] // 4
    sources = ((slabs, 0), (slabs, size), (slabs, size + other), (slabs, size + 2 * other))
    targets = (grad_query, grad_key, grad_value, grad_output)
    wait_all(collect_start(sources, targets, sems))


def tables(segments, size):
    rows = segments.shape[1]
    index_row = jnp.arange(rows)
    same_seg = segments[:, :, None] == segments[:, None, :]
    earlier = index_row[:, None] > index_row[None, :]
    position = jnp.sum(jnp.where(same_seg & earlier, 1, 0), axis=-1)
    frequency = rope_base ** (-2.0 * jnp.arange(size // 2).astype(f32) / size)
    angles = index_row.astype(f32)[:, None] * frequency
    cosine, sine = jnp.cos(angles), jnp.sin(angles)
    first = (index_row - position).reshape(-1, 1)
    return (
        jnp.concatenate([cosine, cosine], axis=1),
        jnp.concatenate([-sine, sine], axis=1),
        jnp.broadcast_to(first, (first.shape[0], rows)).astype(jnp.int32),
    )


def swap(values, axis):
    return lax.ppermute(values, axis, [(0, 1), (1, 0)])


def fetch(spread):
    columns = spread.shape[2]
    return lax.all_gather(spread.reshape(-1, columns), "z", axis=0, tiled=True)


def give_back(grads):
    summed_rows = lax.psum_scatter(grads, "z", scatter_dimension=0, tiled=True)
    return summed_rows.reshape(4, -1, grads.shape[1])


def on_device(depth, tokens, grad_out, segments, attention_gain, query_weight, key_weight,
              value_weight, output_weight, query_gain, key_gain, feedforward_gain, gate_weight,
              up_weight, down_weight):
    size = query_gain.shape[0]
    blocks, rows = segments.shape
    width = tokens.shape[1]
    rows_here = attention_gain.shape[0]
    heads = query_weight.shape[1] // size // 4
    groups = key_weight.shape[1] // size // 4
    counts = (heads, groups, size)
    mine = lax.axis_index("y")
    gain_one, gain_two = attention_gain[:, None], feedforward_gain[:, None]

    def array(dtype, *dims):
        return jax.ShapeDtypeStruct(dims, dtype)

    def scaled(weight, gain):
        return (weight.astype(f32) * gain).astype(bf16)

    def own(values):
        return lax.dynamic_index_in_dim(
            values.reshape(2, -1, values.shape[-1]), mine, 0, keepdims=False
        )

    token_own, grad_own = own(tokens), own(grad_out)
    block_rows = token_own.shape[0]
    block = array(f32, block_rows, width)
    both = array(bf16, 2, block_rows, width)
    everyone = array(bf16, 8, block_rows, width)
    qkv_size = (heads + 2 * groups) * size
    output_size = heads * size
    hidden_size = gate_weight.shape[1] // 4

    def scatter_shapes():
        return scatter_scratch(block_rows, width)

    pairs = segments.reshape(2, -1, rows)
    pairs = jnp.where(mine == 0, pairs, pairs[::-1]).reshape(blocks, rows)
    attention_slabs, segments_all = call(
        enter_kernel,
        1,
        (array(bf16, 4, rows_here, qkv_size + output_size), array(jnp.int32, 4, blocks, rows)),
        sem_pair(16) + sem_pair(4),
        *(scaled(w, gain_one) for w in (query_weight, key_weight, value_weight)),
        output_weight.T,
        pairs,
    )
    attention_all = fetch(attention_slabs)
    qkv_weight = attention_all[:, :qkv_size]
    token_own, _ = lax.optimization_barrier((token_own, segments_all))
    input_one, gate_up_slabs, down_slabs = call(
        tokens_kernel,
        2,
        (
            everyone,
            array(bf16, 4, rows_here, 2 * hidden_size),
            array(bf16, 4, rows_here, hidden_size),
        ),
        sem_pair(14) + sem_pair(12),
        token_own,
        scaled(gate_weight, gain_two),
        scaled(up_weight, gain_two),
        down_weight.T,
    )
    input_one = input_one.reshape(-1, width)
    gate_up_all = fetch(gate_up_slabs)
    down_all = fetch(down_slabs)
    cosine, sine, start = tables(segments_all.reshape(-1, rows), size)
    gains = jnp.stack([query_gain, key_gain])

    qkv = dot(input_one, qkv_weight)
    attended, residual, input_two = call(
        functools.partial(middle_kernel, counts),
        3,
        (array(bf16, 8 * block_rows, output_size), block, everyone),
        [pltpu.VMEM((8, block_rows, width), bf16)] + scatter_shapes() + sem_pair(14),
        qkv,
        cosine,
        sine,
        start,
        gains,
        attention_all,
        token_own,
    )
    input_two = input_two.reshape(-1, width)
    grad_own, _ = lax.optimization_barrier((grad_own, residual))
    grads_all = call(grads_kernel, 4, everyone, sem_pair(14), grad_own).reshape(-1, width)

    gate_up = dot(input_two, gate_up_all)
    gate_pre, up_pre = gate_up[:, :hidden_size], gate_up[:, hidden_size:]
    sigma = jax.nn.sigmoid(gate_pre)
    hidden = (gate_pre * sigma * up_pre).astype(bf16)
    grad_down = dot_tn(grads_all, hidden).astype(bf16)
    _, hidden, gate_pre, up_pre, down_all = lax.optimization_barrier(
        (grad_down, hidden, gate_pre, up_pre, down_all)
    )
    sigma = jax.nn.sigmoid(gate_pre)
    grad_down = give_back(grad_down)
    d_hidden = dot(grads_all, down_all)
    d_gate = (d_hidden * up_pre * sigma * (1.0 + gate_pre * (1.0 - sigma))).astype(bf16)
    d_up = (d_hidden * gate_pre * sigma).astype(bf16)
    d_gate_up = jnp.concatenate([d_gate, d_up], axis=1)
    grad_gate_up = dot_tn(input_two, d_gate_up).astype(bf16)
    grad_gate_up, d_gate_up = lax.optimization_barrier((grad_gate_up, d_gate_up))
    blocks_scratch = pltpu.VMEM((8, block_rows, width), bf16)
    d_residual, d_residual_low = call(
        back_kernel,
        5,
        (block, everyone),
        [blocks_scratch] + scatter_shapes() + sem_pair(14),
        d_gate_up,
        gate_up_all,
        residual,
        grad_own,
    )
    d_residual_low = d_residual_low.reshape(-1, width)
    grad_gate_up = give_back(grad_gate_up)

    grad_output = dot_tn(d_residual_low, attended).astype(bf16)
    d_attended = dot(d_residual_low, attention_all[:, qkv_size:]).astype(bf16)
    d_qkv, gain_sums = pl.pallas_call(
        functools.partial(heads_kernel, counts, block_rows),
        out_shape=(array(bf16, 8 * block_rows, qkv_size), array(f32, 2, size)),
        in_specs=[pl.BlockSpec(memory_space=pltpu.VMEM)] * 6,
        out_specs=(pl.BlockSpec(memory_space=pltpu.VMEM),) * 2,
        compiler_params=pltpu.CompilerParams(vmem_limit_bytes=vmem_limit),
        name="heads",
    )(qkv, cosine, sine, start, gains, d_attended)
    grad_attention = jnp.concatenate(
        [dot_tn(input_one, d_qkv).astype(bf16), grad_output], axis=1
    )
    d_qkv, grad_attention = lax.optimization_barrier((d_qkv, grad_attention))
    grad_attention = give_back(grad_attention)
    stages = 3 + depth.bit_length() - 1
    grad_tokens, mixed_own, head_gains = call(
        functools.partial(leave_kernel, depth),
        7,
        (
            both,
            array(bf16, block_rows, width),
            array(f32, 2, size),
        ),
        [blocks_scratch, blocks_scratch, pltpu.VMEM((block_rows, width), bf16)]
        + scatter_shapes()
        + scatter_shapes()
        + [pltpu.VMEM((stages + 1, 2, size), f32), pltpu.VMEM((stages, 2, size), f32)]
        + sem_pair(stages)
        + sem_pair(2),
        d_qkv,
        attention_all,
        hidden,
        down_all,
        token_own,
        residual,
        d_residual,
        gain_sums,
    )
    raw_gate, raw_up, raw_down, mixed = call(
        gate_up_kernel,
        8,
        (*(array(bf16, rows_here, 4 * hidden_size) for _ in range(3)), both),
        sem_pair(12) + sem_pair(2),
        grad_gate_up,
        grad_down,
        mixed_own,
    )
    grad_attention, _ = lax.optimization_barrier((grad_attention, mixed))
    raw_query, raw_key, raw_value, raw_output = call(
        collect_kernel,
        9,
        (
            array(bf16, *query_weight.shape),
            array(bf16, *key_weight.shape),
            array(bf16, *value_weight.shape),
            array(bf16, rows_here, 4 * output_size),
        ),
        sem_pair(16),
        grad_attention,
    )

    def finish(raw, weights, gain):
        raw = [g.astype(f32) for g in raw]
        sums = sum(jnp.sum(w.astype(f32) * g, axis=1) for w, g in zip(weights, raw))
        sums = sums.reshape(1, rows_here)
        return [g * gain for g in raw], (sums + swap(sums, "y"))[0]

    (grad_query, grad_key, grad_value), grad_one = finish(
        (raw_query, raw_key, raw_value), (query_weight, key_weight, value_weight), gain_one
    )
    (grad_gate, grad_up), grad_two = finish((raw_gate, raw_up), (gate_weight, up_weight), gain_two)
    return (
        mixed.reshape(-1, width),
        grad_tokens.reshape(-1, width).astype(f32),
        grad_one,
        grad_query,
        grad_key,
        grad_value,
        raw_output.T.astype(f32),
        head_gains[0],
        head_gains[1],
        grad_two,
        grad_gate,
        grad_up,
        raw_down.T.astype(f32),
    )


def solution(mesh):
    depth = mesh.shape["fsdp"] // 4
    fine = Mesh(
        mesh.devices.reshape(depth, 2, 2, mesh.shape["tensor"]), ("z", "x", "core", "y")
    )
    fsdp = ("z", "x", "core")
    whole, both, turned, flat = P(fsdp, None), P(fsdp, "y"), P("y", fsdp), P(fsdp)

    def step(*arrays):
        return on_device(depth, *arrays)

    return jax.shard_map(
        step,
        mesh=fine,
        in_specs=(
            whole, whole, whole, flat, both, both, both, turned, P(), P(), flat, both, both, turned
        ),
        out_specs=(
            whole, whole, flat, both, both, both, turned, P(), P(), flat, both, both, turned
        ),
        check_vma=False,
    )
```

```python
import functools

import jax
import jax.numpy as jnp
from jax import lax
from jax.experimental import pallas as pl
from jax.experimental.layout import Layout, with_layout_constraint
from jax.experimental.pallas import tpu as pltpu
from jax.sharding import Mesh
from jax.sharding import PartitionSpec as P


epsilon = 1e-06
rope_base = 1000000.0
bf16 = jnp.bfloat16
f32 = jnp.float32
MESH = pl.DeviceIdType.MESH
chunk = 16
vmem_limit = 40 * 1024 * 1024

bits = {"core": 4, "x": 2, "y": 1}
orders = (("x", "y", "core"), ("y", "x", "core"))
layer = [("core", 1), ("x", 1), ("y", 1)]


def normalize(values):
    inverse = lax.rsqrt(jnp.mean(values * values, axis=-1, keepdims=True) + epsilon)
    return values * inverse, inverse


def norm_back(upstream, normed, inverse):
    return inverse * (upstream - normed * jnp.mean(upstream * normed, axis=-1, keepdims=True))


def dot(left, right):
    return jnp.dot(left, right, preferred_element_type=f32)


def dot_tn(left, right):
    return lax.dot_general(left, right, (((0,), (0,)), ((), ())), preferred_element_type=f32)


def dot_nt(left, right):
    return lax.dot_general(left, right, (((1,), (1,)), ((), ())), preferred_element_type=f32)


def parts_of(width, count):
    tiles = width // 128
    edges = [i * (tiles // count) * 128 for i in range(count)] + [width]
    return [pl.ds(edges[i], edges[i + 1] - edges[i]) for i in range(count)]


def neighbour(axis, step=1):
    return {axis: lax.axis_index(axis) ^ step}


def square_id(step):
    return {"x": lax.axis_index("x") ^ (step >> 1), "core": lax.axis_index("core") ^ (step & 1)}


def square_place(step):
    device = square_id(step)
    return device["x"] * 2 + device["core"]


square = [("core", 1), ("x", 1), ("both", 0)]


def greet(axes):
    barrier = pltpu.get_barrier_semaphore()
    for axis in axes:
        device = square_id(3) if axis[0] == "both" else neighbour(*axis)
        pl.semaphore_signal(barrier, inc=1, device_id=device, device_id_type=MESH)
    pl.semaphore_wait(barrier, len(axes))


def copy_to(device, source, target, sems, number):
    return pltpu.make_async_remote_copy(
        src_ref=source,
        dst_ref=target,
        send_sem=sems[0].at[number],
        recv_sem=sems[1].at[number],
        device_id=device,
        device_id_type=MESH,
    )


def sem_pair(count):
    return [pltpu.SemaphoreType.DMA((count,)), pltpu.SemaphoreType.DMA((count,))]


def over_rows(rows, body):
    def step(i, carry):
        body(pl.ds(pl.multiple_of(i * chunk, chunk), chunk))
        return carry

    lax.fori_loop(0, rows // chunk, step, 0)


def gather_blocks(blocks, sems):
    gather_finish(*gather_start(blocks, sems))


def gather_start(blocks, sems):
    parts = parts_of(blocks.shape[2], len(orders))
    copies = {}

    def send(p, axis, i):
        copies[p, axis, i] = copy_to(
            neighbour(axis),
            blocks.at[i, :, parts[p]],
            blocks.at[i ^ bits[axis], :, parts[p]],
            sems,
            len(copies),
        )
        copies[p, axis, i].start()

    for place in range(3):
        for p, order in enumerate(orders):
            send(p, order[place], 0)
    return copies, send


def gather_finish(copies, send):
    for p, (a, b, c) in enumerate(orders):
        copies[p, a, 0].wait_recv()
        send(p, b, bits[a])
        send(p, c, bits[a])
    for p, (a, b, c) in enumerate(orders):
        copies[p, b, 0].wait_recv()
        send(p, c, bits[b])
        copies[p, b, bits[a]].wait_recv()
        send(p, c, bits[a] ^ bits[b])
    for p, (a, b, c) in enumerate(orders):
        for i in (0, bits[a], bits[b], bits[a] ^ bits[b]):
            copies[p, c, i].wait_recv()
    for copy in copies.values():
        copy.wait_send()


class Scatter:
    def __init__(self, blocks, scratch):
        self.blocks = blocks
        self.first, self.second, self.third, self.sent = scratch[:4]
        self.sems = scratch[4:6]
        self.parts = parts_of(blocks.shape[2], len(orders))
        self.copies = []
        self.arrive = {}

    def send(self, axis, source, target):
        self.copies.append(
            copy_to(neighbour(axis), source, target, self.sems, len(self.copies))
        )
        self.copies[-1].start()
        return self.copies[-1]

    def ready(self, i):
        for p, (a, b, c) in enumerate(orders):
            if i & bits[c]:
                k = (1 if i & bits[a] else 0) + (2 if i & bits[b] else 0)
                self.arrive[p, k] = self.send(
                    c, self.blocks.at[i, :, self.parts[p]], self.first.at[k, :, self.parts[p]]
                )

    def steps(self):
        rows = self.blocks.shape[1]
        blocks, first, second, sent = self.blocks, self.first, self.second, self.sent
        for k in (3, 2):
            for p, (a, b, c) in enumerate(orders):
                j = (bits[a] if k & 1 else 0) ^ bits[b]
                part = self.parts[p]
                self.arrive[p, k].wait_recv()

                def add(row, j=j, k=k, part=part):
                    value = blocks[j, row, part].astype(f32) + first[k, row, part].astype(f32)
                    sent[k - 1, row, part] = value.astype(bf16)

                over_rows(rows, add)
                self.arrive[p, k + 2] = self.send(
                    b, sent.at[k - 1, :, part], second.at[k - 2, :, part]
                )
                yield
        for p, (a, b, c) in enumerate(orders):
            part = self.parts[p]
            self.arrive[p, 1].wait_recv()
            self.arrive[p, 5].wait_recv()

            def add(row, j=bits[a], part=part):
                value = blocks[j, row, part].astype(f32) + first[1, row, part].astype(f32)
                value = value + second[1, row, part].astype(f32)
                sent[0, row, part] = value.astype(bf16)

            over_rows(rows, add)
            self.arrive[p, 6] = self.send(a, sent.at[0, :, part], self.third.at[0, :, part])
            yield
        for p in range(len(orders)):
            for k in (0, 4, 6):
                self.arrive[p, k].wait_recv()
        for copy in self.copies:
            copy.wait_send()

    def run(self):
        for _ in self.steps():
            pass

    def row(self, row):
        value = self.blocks[0, row].astype(f32) + self.first[0, row].astype(f32)
        return value + self.second[0, row].astype(f32) + self.third[0, row].astype(f32)


def products(scatter, left, right, columns):
    rows = scatter.blocks.shape[1]

    def step(i, carry):
        row = pl.ds(pl.multiple_of(i * rows, rows), rows)
        scatter.blocks[i] = dot_nt(left[row], right[:, columns]).astype(bf16)
        return carry

    lax.fori_loop(0, 8, step, 0)
    for i in range(4, 8):
        scatter.ready(i)


def scatter_scratch(rows, width):
    return [
        pltpu.VMEM((4, rows, width), bf16),
        pltpu.VMEM((2, rows, width), bf16),
        pltpu.VMEM((1, rows, width), bf16),
        pltpu.VMEM((3, rows, width), bf16),
        *sem_pair(7 * len(orders)),
    ]


def call(kernel, number, outputs, scratch, *operands):
    return pl.pallas_call(
        kernel,
        out_shape=outputs,
        in_specs=[pl.BlockSpec(memory_space=pltpu.VMEM)] * len(operands),
        out_specs=jax.tree.map(lambda _: pl.BlockSpec(memory_space=pltpu.VMEM), outputs),
        scratch_shapes=scratch,
        compiler_params=pltpu.CompilerParams(
            collective_id=number, has_side_effects=True, vmem_limit_bytes=vmem_limit
        ),
    )(*operands)


def start_all(copies):
    for copy in copies:
        copy.start()
    return copies


def wait_all(copies):
    for copy in copies:
        copy.wait()


def spread_start(sources, targets, sems, number=0):
    me = square_place(0)
    copies = []
    for source, (target, at) in zip(sources, targets):
        size = source.shape[1] // 4
        into = target.at[me, :, pl.ds(at, size)]

        def piece(place, source=source, size=size):
            return source.at[:, pl.ds(pl.multiple_of(place * size, size), size)]

        for step in (3, 1, 2):
            away = piece(square_place(step))
            copies.append(copy_to(square_id(step), away, into, sems, number + step))
        copies.append(pltpu.make_async_copy(piece(me), into, sems[0].at[number]))
        number += 4
    return start_all(copies)


def collect_start(sources, targets, sems):
    me = square_place(0)
    copies = []
    for number, ((source, at), target) in enumerate(zip(sources, targets)):
        size = target.shape[1] // 4
        into = target.at[:, pl.ds(pl.multiple_of(me * size, size), size)]
        for step in (3, 1, 2):
            away = source.at[square_place(step), :, pl.ds(at, size)]
            copies.append(copy_to(square_id(step), away, into, sems, number * 4 + step))
        copies.append(
            pltpu.make_async_copy(source.at[me, :, pl.ds(at, size)], into, sems[0].at[number * 4])
        )
    return start_all(copies)


def enter_kernel(query, key, value, output, slabs, *sems):
    greet(square)
    size, other = query.shape[1] // 4, key.shape[1] // 4
    targets = [(slabs, at) for at in (0, size, size + other, size + 2 * other)]
    wait_all(spread_start((query, key, value, output), targets, sems))


def tokens_kernel(tokens, gate, up, down, segments, inputs_all, gate_up_slabs, down_slabs,
                  segments_all, *sems):
    greet(square + [("y", 1)])

    def norm(row):
        normed, _ = normalize(tokens[row].astype(f32))
        inputs_all[0, row] = normed.astype(bf16)

    over_rows(tokens.shape[0], norm)
    hidden = gate.shape[1] // 4
    targets = ((gate_up_slabs, 0), (gate_up_slabs, hidden), (down_slabs, 0))
    gather = gather_start(inputs_all, sems[:2])
    copies = spread_start((gate, up, down), targets, sems[2:4])
    segments_all[0] = segments[...]
    copies += start_all(
        [
            copy_to(
                square_id(step),
                segments,
                segments_all.at[step // 2 + step % 2 * 2],
                sems[4:],
                step,
            )
            for step in (1, 2, 3)
        ]
    )
    gather_finish(*gather)
    wait_all(copies)


def grads_kernel(grads, grads_all, *sems):
    greet(layer)
    grads_all[0] = grads[...]
    gather_blocks(grads_all, sems)


def turn(value, cosine, sine):
    return value * cosine + pltpu.roll(value, value.shape[1] // 2, 1) * sine


def block_tables(start, cosine, sine):
    rows = lax.broadcasted_iota(jnp.int32, start.shape, 0)
    columns = lax.broadcasted_iota(jnp.int32, start.shape, 1)
    pick = jnp.where(columns == rows - start, 1.0, 0.0)
    cos, sin = (
        jnp.dot(pick, table[...], precision=lax.Precision.HIGHEST, preferred_element_type=f32)
        for table in (cosine, sine)
    )
    return (columns >= start) & (columns <= rows), cos, sin


def probabilities(queries, keys, allowed):
    scores = dot_nt(queries, keys) * queries.shape[1] ** (-0.5)
    scores = jnp.where(allowed, scores, -1e30)
    powers = jnp.exp(scores - jnp.max(scores, axis=1, keepdims=True))
    return powers / jnp.sum(powers, axis=1, keepdims=True)


def head_columns(heads, groups, size):
    query = [pl.ds(h * size, size) for h in range(heads)]
    key = [pl.ds((heads + g) * size, size) for g in range(groups)]
    value = [pl.ds((heads + groups + g) * size, size) for g in range(groups)]
    return query, key, value


def middle_kernel(counts, qkv, cosine, sine, start, gains, output, tokens, attended,
                  residual, inputs_all, partial, *scratch):
    greet(layer)
    heads, groups, size = counts
    rows = tokens.shape[0]
    query, key, value = head_columns(heads, groups, size)
    total = Scatter(partial, scratch[:6])

    def attend(i, carry):
        row = pl.ds(pl.multiple_of(i * rows, rows), rows)
        allowed, cos, sin = block_tables(start[row], cosine, sine)
        for g in range(groups):
            keys = turn(normalize(qkv[row, key[g]])[0] * gains[1:2], cos, sin).astype(bf16)
            values = qkv[row, value[g]].astype(bf16)
            for h in range(g * (heads // groups), (g + 1) * (heads // groups)):
                queries = normalize(qkv[row, query[h]])[0] * gains[0:1]
                queries = turn(queries, cos, sin).astype(bf16)
                probs = probabilities(queries, keys, allowed)
                attended[row, query[h]] = dot(probs.astype(bf16), values).astype(bf16)
        return carry

    lax.fori_loop(0, 8, attend, 0)
    products(total, attended, output, pl.ds(output.shape[1] - heads * size, heads * size))
    total.run()

    def norm(row):
        value = total.row(row) + tokens[row].astype(f32)
        residual[row] = value
        inputs_all[0, row] = normalize(value)[0].astype(bf16)

    over_rows(rows, norm)
    gather_blocks(inputs_all, scratch[6:8])


def back_kernel(d_gate_up, gate_up, residual, grads, d_residual, low_all, partial, *scratch):
    greet(layer)
    total = Scatter(partial, scratch[:6])
    products(total, d_gate_up, gate_up, slice(None))
    total.run()

    def norm(row):
        normed, inverse = normalize(residual[row])
        value = grads[row].astype(f32) + norm_back(total.row(row), normed, inverse)
        d_residual[row] = value
        low_all[0, row] = value.astype(bf16)

    over_rows(residual.shape[0], norm)
    gather_blocks(low_all, scratch[6:8])


def share_start(own, both, sems):
    mine = lax.axis_index("y")
    return start_all(
        [
            copy_to(neighbour("y"), own, both.at[mine], sems, 0),
            pltpu.make_async_copy(own, both.at[mine], sems[0].at[1]),
        ]
    )


def heads_kernel(counts, rows, qkv, cosine, sine, start, gains, d_attended, d_qkv, gain_sums):
    heads, groups, size = counts
    scale = size ** (-0.5)
    query, key, value = head_columns(heads, groups, size)

    def block(i, sums):
        query_sum, key_sum = sums
        row = pl.ds(pl.multiple_of(i * rows, rows), rows)
        allowed, cos, sin = block_tables(start[row], cosine, sine)
        for g in range(groups):
            key_hat, key_inverse = normalize(qkv[row, key[g]])
            keys = turn(key_hat * gains[1:2], cos, sin).astype(bf16)
            values = qkv[row, value[g]].astype(bf16)
            d_keys = d_values = 0.0
            for h in range(g * (heads // groups), (g + 1) * (heads // groups)):
                query_hat, query_inverse = normalize(qkv[row, query[h]])
                queries = turn(query_hat * gains[0:1], cos, sin).astype(bf16)
                probs = probabilities(queries, keys, allowed)
                upstream = d_attended[row, query[h]]
                d_values = d_values + dot_tn(probs.astype(bf16), upstream)
                d_probs = dot_nt(upstream, values)
                inner = jnp.sum(d_probs * probs, axis=1, keepdims=True)
                d_scores = (probs * (d_probs - inner)).astype(bf16)
                d_keys = d_keys + dot_tn(d_scores, queries)
                d_query = turn(dot(d_scores, keys) * scale, cos, -sin)
                query_sum = query_sum + jnp.sum(d_query * query_hat, axis=0, keepdims=True)
                d_qkv[row, query[h]] = norm_back(
                    d_query * gains[0:1], query_hat, query_inverse
                ).astype(bf16)
            d_key = turn(d_keys * scale, cos, -sin)
            key_sum = key_sum + jnp.sum(d_key * key_hat, axis=0, keepdims=True)
            d_qkv[row, key[g]] = norm_back(d_key * gains[1:2], key_hat, key_inverse).astype(bf16)
            d_qkv[row, value[g]] = d_values.astype(bf16)
        return query_sum, key_sum

    zeros = jnp.zeros((1, size), f32)
    query_sum, key_sum = lax.fori_loop(0, 8, block, (zeros, zeros))
    gain_sums[0:1] = query_sum
    gain_sums[1:2] = key_sum


def leave_kernel(depth, d_qkv, weights, hidden, down, tokens, residual, d_residual, gain_sums,
                 grad_tokens, mixed_own, gain_totals, partial, mixed_partial, token_grads, *scratch):
    stages = layer + [("z", 1 << n) for n in range(depth.bit_length() - 1)]
    greet(stages)
    total = Scatter(partial, scratch[:6])
    other = Scatter(mixed_partial, scratch[6:12])
    products(total, d_qkv, weights, pl.ds(0, d_qkv.shape[1]))
    products(other, hidden, down, slice(None))
    held, arrived, sems = scratch[12], scratch[13], scratch[14:16]
    held[0] = gain_sums[...]
    ticks = total.steps()
    for n, axis in enumerate(stages):
        copy = copy_to(neighbour(*axis), held.at[n], arrived.at[n], sems, n)
        copy.start()
        next(ticks, None)
        copy.wait()
        held[n + 1] = held[n] + arrived[n]
    gain_totals[...] = held[len(stages)]
    other_ticks = other.steps()
    for _ in ticks:
        next(other_ticks, None)

    def norm(row):
        normed, inverse = normalize(tokens[row].astype(f32))
        value = d_residual[row] + norm_back(total.row(row), normed, inverse)
        token_grads[row] = value.astype(bf16)

    over_rows(tokens.shape[0], norm)
    shared = share_start(token_grads, grad_tokens, scratch[16:18])
    for _ in other_ticks:
        pass

    def add(row):
        mixed_own[row] = (residual[row] + other.row(row)).astype(bf16)

    over_rows(tokens.shape[0], add)
    wait_all(shared)


def gate_up_kernel(slabs, down_slabs, mixed_own, grad_gate, grad_up, grad_down, mixed, *sems):
    greet(square + [("y", 1)])
    shared = share_start(mixed_own, mixed, sems[2:])
    sources = ((slabs, 0), (slabs, grad_gate.shape[1] // 4), (down_slabs, 0))
    wait_all(collect_start(sources, (grad_gate, grad_up, grad_down), sems[:2]))
    wait_all(shared)


def collect_kernel(slabs, grad_query, grad_key, grad_value, grad_output, *sems):
    greet(square)
    size, other = grad_query.shape[1] // 4, grad_key.shape[1] // 4
    sources = ((slabs, 0), (slabs, size), (slabs, size + other), (slabs, size + 2 * other))
    targets = (grad_query, grad_key, grad_value, grad_output)
    wait_all(collect_start(sources, targets, sems))


def tables(segments, size):
    rows = segments.shape[1]
    index_row = jnp.arange(rows)
    same_seg = segments[:, :, None] == segments[:, None, :]
    earlier = index_row[:, None] > index_row[None, :]
    position = jnp.sum(jnp.where(same_seg & earlier, 1, 0), axis=-1)
    frequency = rope_base ** (-2.0 * jnp.arange(size // 2).astype(f32) / size)
    angles = index_row.astype(f32)[:, None] * frequency
    cosine, sine = jnp.cos(angles), jnp.sin(angles)
    first = (index_row - position).reshape(-1, 1)
    return (
        jnp.concatenate([cosine, cosine], axis=1),
        jnp.concatenate([-sine, sine], axis=1),
        jnp.broadcast_to(first, (first.shape[0], rows)).astype(jnp.int32),
    )


def swap(values, axis):
    return lax.ppermute(values, axis, [(0, 1), (1, 0)])


def fetch(spread):
    columns = spread.shape[2]
    return lax.all_gather(spread.reshape(-1, columns), "z", axis=0, tiled=True)


def give_back(grads):
    summed_rows = lax.psum_scatter(grads, "z", scatter_dimension=0, tiled=True)
    return summed_rows.reshape(4, -1, grads.shape[1])


def on_device(depth, tokens, grad_out, segments, attention_gain, query_weight, key_weight,
              value_weight, output_weight, query_gain, key_gain, feedforward_gain, gate_weight,
              up_weight, down_weight):
    size = query_gain.shape[0]
    blocks, rows = segments.shape
    width = tokens.shape[1]
    rows_here = attention_gain.shape[0]
    heads = query_weight.shape[1] // size // 4
    groups = key_weight.shape[1] // size // 4
    counts = (heads, groups, size)
    mine = lax.axis_index("y")
    gain_one, gain_two = attention_gain[:, None], feedforward_gain[:, None]

    def array(dtype, *dims):
        return jax.ShapeDtypeStruct(dims, dtype)

    def scaled(weight, gain):
        return (weight.astype(f32) * gain).astype(bf16)

    def own(values):
        return lax.dynamic_index_in_dim(
            values.reshape(2, -1, values.shape[-1]), mine, 0, keepdims=False
        )

    token_own, grad_own = own(tokens), own(grad_out)
    block_rows = token_own.shape[0]
    block = array(f32, block_rows, width)
    both = array(bf16, 2, block_rows, width)
    everyone = array(bf16, 8, block_rows, width)
    qkv_size = (heads + 2 * groups) * size
    output_size = heads * size
    hidden_size = gate_weight.shape[1] // 4

    def scatter_shapes():
        return scatter_scratch(block_rows, width)

    attention_slabs = call(
        enter_kernel,
        1,
        array(bf16, 4, rows_here, qkv_size + output_size),
        sem_pair(16),
        *(scaled(w, gain_one) for w in (query_weight, key_weight, value_weight)),
        output_weight.T,
    )
    attention_all = fetch(attention_slabs)
    qkv_weight = attention_all[:, :qkv_size]
    token_own, segments, _ = lax.optimization_barrier((token_own, segments, attention_slabs))
    pairs = segments.reshape(2, -1, rows)
    pairs = jnp.where(mine == 0, pairs, pairs[::-1]).reshape(blocks, rows)
    input_one, gate_up_slabs, down_slabs, segments_all = call(
        tokens_kernel,
        2,
        (
            everyone,
            array(bf16, 4, rows_here, 2 * hidden_size),
            array(bf16, 4, rows_here, hidden_size),
            array(jnp.int32, 4, blocks, rows),
        ),
        sem_pair(14) + sem_pair(12) + sem_pair(4),
        token_own,
        scaled(gate_weight, gain_two),
        scaled(up_weight, gain_two),
        down_weight.T,
        pairs,
    )
    input_one = input_one.reshape(-1, width)
    gate_up_all = fetch(gate_up_slabs)
    down_all = fetch(down_slabs)
    cosine, sine, start = tables(segments_all.reshape(-1, rows), size)
    gains = jnp.stack([query_gain, key_gain])

    qkv = dot(input_one, qkv_weight)
    attended, residual, input_two = call(
        functools.partial(middle_kernel, counts),
        3,
        (array(bf16, 8 * block_rows, output_size), block, everyone),
        [pltpu.VMEM((8, block_rows, width), bf16)] + scatter_shapes() + sem_pair(14),
        qkv,
        cosine,
        sine,
        start,
        gains,
        attention_all,
        token_own,
    )
    input_two = input_two.reshape(-1, width)
    grad_own, _ = lax.optimization_barrier((grad_own, residual))
    grads_all = call(grads_kernel, 4, everyone, sem_pair(14), grad_own).reshape(-1, width)

    gate_up = dot(input_two, gate_up_all)
    gate_pre, up_pre = gate_up[:, :hidden_size], gate_up[:, hidden_size:]
    sigma = jax.nn.sigmoid(gate_pre)
    hidden = (gate_pre * sigma * up_pre).astype(bf16)
    grad_down = dot_tn(grads_all, hidden).astype(bf16)
    _, hidden, gate_pre, up_pre, down_all = lax.optimization_barrier(
        (grad_down, hidden, gate_pre, up_pre, down_all)
    )
    sigma = jax.nn.sigmoid(gate_pre)
    grad_down = give_back(grad_down)
    d_hidden = dot(grads_all, down_all)
    d_gate = (d_hidden * up_pre * sigma * (1.0 + gate_pre * (1.0 - sigma))).astype(bf16)
    d_up = (d_hidden * gate_pre * sigma).astype(bf16)
    d_gate_up = jnp.concatenate([d_gate, d_up], axis=1)
    grad_gate_up = dot_tn(input_two, d_gate_up).astype(bf16)
    grad_gate_up, d_gate_up = lax.optimization_barrier((grad_gate_up, d_gate_up))
    blocks_scratch = pltpu.VMEM((8, block_rows, width), bf16)
    d_residual, d_residual_low = call(
        back_kernel,
        5,
        (block, everyone),
        [blocks_scratch] + scatter_shapes() + sem_pair(14),
        d_gate_up,
        gate_up_all,
        residual,
        grad_own,
    )
    d_residual_low = d_residual_low.reshape(-1, width)
    grad_gate_up = give_back(grad_gate_up)

    grad_output = dot_tn(d_residual_low, attended).astype(bf16)
    d_attended = dot(d_residual_low, attention_all[:, qkv_size:]).astype(bf16)
    d_qkv, gain_sums = pl.pallas_call(
        functools.partial(heads_kernel, counts, block_rows),
        out_shape=(array(bf16, 8 * block_rows, qkv_size), array(f32, 2, size)),
        in_specs=[pl.BlockSpec(memory_space=pltpu.VMEM)] * 6,
        out_specs=(pl.BlockSpec(memory_space=pltpu.VMEM),) * 2,
        compiler_params=pltpu.CompilerParams(vmem_limit_bytes=vmem_limit),
        name="heads",
    )(qkv, cosine, sine, start, gains, d_attended)
    grad_attention = jnp.concatenate(
        [dot_tn(input_one, d_qkv).astype(bf16), grad_output], axis=1
    )
    d_qkv, grad_attention = lax.optimization_barrier((d_qkv, grad_attention))
    grad_attention = with_layout_constraint(grad_attention, Layout((0, 1)))
    grad_attention = give_back(grad_attention)
    stages = 3 + depth.bit_length() - 1
    grad_tokens, mixed_own, head_gains = call(
        functools.partial(leave_kernel, depth),
        7,
        (
            both,
            array(bf16, block_rows, width),
            array(f32, 2, size),
        ),
        [blocks_scratch, blocks_scratch, pltpu.VMEM((block_rows, width), bf16)]
        + scatter_shapes()
        + scatter_shapes()
        + [pltpu.VMEM((stages + 1, 2, size), f32), pltpu.VMEM((stages, 2, size), f32)]
        + sem_pair(stages)
        + sem_pair(2),
        d_qkv,
        attention_all,
        hidden,
        down_all,
        token_own,
        residual,
        d_residual,
        gain_sums,
    )
    raw_gate, raw_up, raw_down, mixed = call(
        gate_up_kernel,
        8,
        (*(array(bf16, rows_here, 4 * hidden_size) for _ in range(3)), both),
        sem_pair(12) + sem_pair(2),
        grad_gate_up,
        grad_down,
        mixed_own,
    )
    grad_attention, _ = lax.optimization_barrier((grad_attention, mixed))
    raw_query, raw_key, raw_value, raw_output = call(
        collect_kernel,
        9,
        (
            array(bf16, *query_weight.shape),
            array(bf16, *key_weight.shape),
            array(bf16, *value_weight.shape),
            array(bf16, rows_here, 4 * output_size),
        ),
        sem_pair(16),
        grad_attention,
    )

    def finish(raw, weights, gain):
        raw = [g.astype(f32) for g in raw]
        sums = sum(jnp.sum(w.astype(f32) * g, axis=1) for w, g in zip(weights, raw))
        sums = sums.reshape(1, rows_here)
        return [g * gain for g in raw], (sums + swap(sums, "y"))[0]

    (grad_query, grad_key, grad_value), grad_one = finish(
        (raw_query, raw_key, raw_value), (query_weight, key_weight, value_weight), gain_one
    )
    (grad_gate, grad_up), grad_two = finish((raw_gate, raw_up), (gate_weight, up_weight), gain_two)
    return (
        mixed.reshape(-1, width),
        grad_tokens.reshape(-1, width).astype(f32),
        grad_one,
        grad_query,
        grad_key,
        grad_value,
        raw_output.T.astype(f32),
        head_gains[0],
        head_gains[1],
        grad_two,
        grad_gate,
        grad_up,
        raw_down.T.astype(f32),
    )


def solution(mesh):
    depth = mesh.shape["fsdp"] // 4
    fine = Mesh(
        mesh.devices.reshape(depth, 2, 2, mesh.shape["tensor"]), ("z", "x", "core", "y")
    )
    fsdp = ("z", "x", "core")
    whole, both, turned, flat = P(fsdp, None), P(fsdp, "y"), P("y", fsdp), P(fsdp)

    def step(*arrays):
        return on_device(depth, *arrays)

    return jax.shard_map(
        step,
        mesh=fine,
        in_specs=(
            whole, whole, whole, flat, both, both, both, turned, P(), P(), flat, both, both, turned
        ),
        out_specs=(
            whole, whole, flat, both, both, both, turned, P(), P(), flat, both, both, turned
        ),
        check_vma=False,
    )
```
